16 devices in a mesh: dp: 2 (over y, z), ep: 8 (over x, core).
Axes of the slice: x: 4, y: 2, z: 1, core: 2. Of those that a mesh axis runs over, the one named last changes fastest.
The devices are a block of a 4x4x8 slice.
Arguments:
- x_a: bfloat16 [2048, 2560], P(('dp', 'ep')), parts along dimension 0
- route_a: int32 [2048, 6], P(('dp', 'ep')), parts along dimension 0
- gate_a: float32 [2048, 6], P(('dp', 'ep')), parts along dimension 0
- h_b: bfloat16 [2048, 2560], P(('dp', 'ep')), parts along dimension 0
- attn_b: bfloat16 [2048, 2560], P(('dp', 'ep')), parts along dimension 0
- route_b: int32 [2048, 6], P(('dp', 'ep')), parts along dimension 0
- gate_b: float32 [2048, 6], P(('dp', 'ep')), parts along dimension 0
- w_qkv: bfloat16 [2560, 3584], replicated
- w_o: bfloat16 [2560, 2560], replicated
- w_gate: bfloat16 [64, 2560, 1536], P('ep')
- w_up: bfloat16 [64, 2560, 1536], P('ep')
- w_down: bfloat16 [64, 1536, 2560], P('ep')
Outputs:
- output 1: bfloat16 [2048, 2560], P(('dp', 'ep')), parts along dimension 0
- output 2: bfloat16 [2048, 2560], P(('dp', 'ep')), parts along dimension 0
- output 3: bfloat16 [2048, 3584], P(('dp', 'ep')), parts along dimension 0
There are 2 independent parts. The reference program is written for one: setup_inputs(seed, part) draws one part's arguments, and reference() takes and returns one part's arrays. A program takes and returns all parts, laid end to end along the dimension named above; an argument that names none is the same for every part.
All inputs are finite; a program needn't handle non-finite values.
Results may differ from the reference program's by a relative error of at most 0.0110739.
Values are sent between devices in bfloat16 or wider.
A program may use at most 768 MiB of HBM per device.

```python
import jax
import jax.numpy as jnp
from jax import lax

MODEL_DIM = 2560
FF_DIM = 1536
NUM_EXPERTS = 64
TOP_K = 6
NUM_HEADS = 20
KV_HEADS = 4
HEAD_DIM = 128
TOKENS_DEV = 128
GROUP_DEVS = 8

CAPACITY = min(TOKENS_DEV, 2 * ((TOKENS_DEV * TOP_K + NUM_EXPERTS - 1) // NUM_EXPERTS))
LOCAL_EXPERTS = NUM_EXPERTS // GROUP_DEVS
QKV_DIM = (NUM_HEADS + 2 * KV_HEADS) * HEAD_DIM
ATTN_DIM = NUM_HEADS * HEAD_DIM
GROUP_ROWS = GROUP_DEVS * TOKENS_DEV
HOT_DEVS = max(1, GROUP_DEVS // 4)


def source_routing(rng_key, dev_order):
    key_local, key_want, key_rows = jax.random.split(rng_key, 3)
    local_order = jax.vmap(lambda sub_key: jax.random.permutation(sub_key, LOCAL_EXPERTS))(jax.random.split(key_local, GROUP_DEVS))
    visits = jnp.arange(NUM_EXPERTS)
    visit_dev = dev_order[visits % GROUP_DEVS]
    visit_expert = visit_dev * LOCAL_EXPERTS + local_order[visit_dev, visits // GROUP_DEVS]
    wanted = jax.random.randint(key_want, (NUM_EXPERTS,), 1, CAPACITY + 1)
    wanted = jnp.where(visits % GROUP_DEVS < HOT_DEVS, CAPACITY, wanted)
    wanted = jnp.where(visits < GROUP_DEVS, 1, wanted)
    wanted = jnp.where(visits == 0, CAPACITY, wanted)
    n_entries = TOKENS_DEV * TOP_K
    first_pass = jnp.clip(n_entries - (jnp.cumsum(wanted) - wanted), 0, wanted)
    room_left = CAPACITY - first_pass
    left_over = n_entries - jnp.sum(first_pass)
    second_pass = jnp.clip(left_over - (jnp.cumsum(room_left) - room_left), 0, room_left)
    run_ends = jnp.cumsum(first_pass + second_pass)
    positions = jnp.arange(n_entries)
    run_index = jnp.sum((run_ends[None, :] <= positions[:, None]).astype(jnp.int32), axis=1)
    choices = visit_expert[run_index].reshape(TOP_K, TOKENS_DEV).T
    return choices[jax.random.permutation(key_rows, TOKENS_DEV)]


def group_routing(rng_key):
    key_order, key_src = jax.random.split(rng_key)
    dev_order = jax.random.permutation(key_order, GROUP_DEVS)
    per_source = jax.vmap(lambda sub_key: source_routing(sub_key, dev_order))(jax.random.split(key_src, GROUP_DEVS))
    return per_source.reshape(GROUP_ROWS, TOP_K).astype(jnp.int32)


def setup_inputs(seed: int = 0, part: int = 0) -> dict:
    root_key = jax.random.key(seed)
    shared_keys = jax.random.split(jax.random.fold_in(root_key, 1), 5)
    part_keys = jax.random.split(jax.random.fold_in(jax.random.fold_in(root_key, 2), part), 7)

    def normal_bf16(sub_key, arr_shape, scale_by):
        return (jax.random.normal(sub_key, arr_shape, jnp.float32) * scale_by).astype(jnp.bfloat16)

    return {
        'x_a': normal_bf16(part_keys[0], (GROUP_ROWS, MODEL_DIM), 1.0),
        'route_a': group_routing(part_keys[1]),
        'gate_a': jax.nn.softmax(jax.random.normal(part_keys[2], (GROUP_ROWS, TOP_K), jnp.float32), axis=-1),
        'h_b': normal_bf16(part_keys[3], (GROUP_ROWS, MODEL_DIM), 1.0),
        'attn_b': normal_bf16(part_keys[4], (GROUP_ROWS, ATTN_DIM), 1.0),
        'route_b': group_routing(part_keys[5]),
        'gate_b': jax.nn.softmax(jax.random.normal(part_keys[6], (GROUP_ROWS, TOP_K), jnp.float32), axis=-1),
        'w_qkv': normal_bf16(shared_keys[0], (MODEL_DIM, QKV_DIM), MODEL_DIM ** -0.5),
        'w_o': normal_bf16(shared_keys[1], (ATTN_DIM, MODEL_DIM), ATTN_DIM ** -0.5),
        'w_gate': normal_bf16(shared_keys[2], (NUM_EXPERTS, MODEL_DIM, FF_DIM), MODEL_DIM ** -0.5),
        'w_up': normal_bf16(shared_keys[3], (NUM_EXPERTS, MODEL_DIM, FF_DIM), MODEL_DIM ** -0.5),
        'w_down': normal_bf16(shared_keys[4], (NUM_EXPERTS, FF_DIM, MODEL_DIM), FF_DIM ** -0.5),
    }


def expert_layer(tokens, route_ids, gate_vals, w_gate, w_up, w_down):
    n_entries = GROUP_ROWS * TOP_K
    per_source = route_ids.reshape(GROUP_DEVS, TOKENS_DEV * TOP_K)
    one_hot = (per_source[:, :, None] == jnp.arange(NUM_EXPERTS)[None, None, :]).astype(jnp.int32)
    slot_rank = jnp.sum((jnp.cumsum(one_hot, axis=1) - 1) * one_hot, axis=2)
    buffer_row = jnp.arange(GROUP_DEVS)[:, None] * CAPACITY + slot_rank
    entry_ids = jnp.arange(n_entries)
    slot_table = jnp.full((NUM_EXPERTS, GROUP_DEVS * CAPACITY), n_entries, jnp.int32)
    slot_table = slot_table.at[per_source.reshape(-1), buffer_row.reshape(-1)].set(entry_ids)
    padded = jnp.concatenate([tokens, jnp.zeros((1, MODEL_DIM), tokens.dtype)], axis=0)

    def one_expert(results, inputs):
        rows_ids, gate_w, up_w, down_w = inputs
        expert_in = padded[rows_ids // TOP_K]
        gate_act = jnp.dot(expert_in, gate_w, preferred_element_type=jnp.float32)
        up_act = jnp.dot(expert_in, up_w, preferred_element_type=jnp.float32)
        hidden = (jax.nn.silu(gate_act) * up_act).astype(jnp.bfloat16)
        expert_out = jnp.dot(hidden, down_w, preferred_element_type=jnp.float32).astype(jnp.bfloat16)
        return results.at[rows_ids].set(expert_out), None

    results = jnp.zeros((n_entries + 1, MODEL_DIM), jnp.bfloat16)
    results = lax.scan(one_expert, results, (slot_table, w_gate, w_up, w_down))[0]
    per_choice = results[:n_entries].reshape(GROUP_ROWS, TOP_K, MODEL_DIM)
    mixture = jnp.zeros((GROUP_ROWS, MODEL_DIM), jnp.float32)
    for choice in range(TOP_K):
        mixture = mixture + gate_vals[:, choice:choice + 1] * per_choice[:, choice].astype(jnp.float32)
    return (tokens.astype(jnp.float32) + mixture).astype(jnp.bfloat16)


def reference(x_a, route_a, gate_a, h_b, attn_b, route_b, gate_b, w_qkv, w_o, w_gate, w_up, w_down):
    out_a = expert_layer(x_a, route_a, gate_a, w_gate, w_up, w_down)
    qkv_b = jnp.dot(h_b, w_qkv, preferred_element_type=jnp.float32).astype(jnp.bfloat16)
    proj_b = jnp.dot(attn_b, w_o, preferred_element_type=jnp.float32).astype(jnp.bfloat16)
    mid_b = (h_b.astype(jnp.float32) + proj_b.astype(jnp.float32)).astype(jnp.bfloat16)
    out_b = expert_layer(mid_b, route_b, gate_b, w_gate, w_up, w_down)
    return (out_a, out_b, qkv_b)
```

```python
import functools

import jax
import jax.numpy as jnp
from jax import lax
from jax.experimental import pallas as pl
from jax.experimental.pallas import tpu as pltpu
from jax.sharding import PartitionSpec as P

F32 = jnp.float32
BF16 = jnp.bfloat16


def slot_map(routes, gates, first_expert, local_n, cap):
    n_src, tok_n, _ = routes.shape
    ids = first_expert + jnp.arange(local_n)
    hit = routes[:, None, :, :] == ids[None, :, None, None]
    member = jnp.any(hit, axis=3)
    gate = jnp.sum(jnp.where(hit, gates[:, None, :, :], 0.0), axis=3)
    tri = (jnp.arange(tok_n)[:, None] < jnp.arange(tok_n)[None, :]).astype(BF16)
    rank = jnp.einsum('sek,kt->set', member.astype(BF16), tri, preferred_element_type=F32).astype(jnp.int32)
    half = (jnp.arange(n_src) % 2)[:, None, None] * cap
    slot = jnp.where(member, rank + half, -1)

    def pair_up(a):
        return a.reshape(n_src // 2, 2, local_n, tok_n).transpose(0, 2, 1, 3).reshape(n_src // 2, local_n, 2 * tok_n)

    return pair_up(slot), pair_up(gate)


def pick(slot_row, n_slots):
    return lax.broadcasted_iota(jnp.int32, (n_slots, slot_row.shape[-1]), 0) == slot_row


def gate_up_kernel(cap2, x_ref, slot_ref, wg_ref, wu_ref, h_ref, rows):
    n_pair, local_n, width = slot_ref.shape

    @pl.when((pl.program_id(0) == 0) & (pl.program_id(1) == 0))
    def _():
        for p in range(n_pair):
            sel = jnp.concatenate([jnp.where(pick(slot_ref[p, e:e + 1, :], cap2), 1.0, 0.0) for e in range(local_n)], axis=0)
            got = jnp.dot(sel.astype(BF16), x_ref[p * width:(p + 1) * width, :], preferred_element_type=F32).astype(BF16)
            for e in range(local_n):
                rows[e, p * cap2:(p + 1) * cap2, :] = got[e * cap2:(e + 1) * cap2, :]

    mine = rows[pl.program_id(0)]
    gate = jnp.dot(mine, wg_ref[0], preferred_element_type=F32)
    up = jnp.dot(mine, wu_ref[0], preferred_element_type=F32)
    h_ref[0] = (jax.nn.silu(gate) * up).astype(BF16)


def gate_up(x_all, slot, w_gate, w_up, cap, fc=512):
    local_n, dim, ff = w_gate.shape
    n_pair = slot.shape[0]
    m = n_pair * 2 * cap
    return pl.pallas_call(
        functools.partial(gate_up_kernel, 2 * cap),
        out_shape=jax.ShapeDtypeStruct((local_n, m, ff), BF16),
        grid=(local_n, ff // fc),
        in_specs=[
            pl.BlockSpec(x_all.shape, lambda e, f: (0, 0)),
            pl.BlockSpec(slot.shape, lambda e, f: (0, 0, 0)),
            pl.BlockSpec((1, dim, fc), lambda e, f: (e, 0, f)),
            pl.BlockSpec((1, dim, fc), lambda e, f: (e, 0, f)),
        ],
        out_specs=pl.BlockSpec((1, m, fc), lambda e, f: (e, 0, f)),
        scratch_shapes=[pltpu.VMEM((local_n, m, dim), BF16)],
        compiler_params=pltpu.CompilerParams(vmem_limit_bytes=56 * 2 ** 20),
        cost_estimate=pl.CostEstimate(flops=4 * local_n * m * dim * ff, bytes_accessed=4 * local_n * dim * ff, transcendentals=0),
    )(x_all, slot, w_gate, w_up)


def down_kernel(cap2, slot_ref, gate_ref, h_ref, wd_ref, o_ref, ys):
    n_pair, local_n, width = slot_ref.shape
    e = pl.program_id(0)
    y = jnp.dot(h_ref[e], wd_ref[0], preferred_element_type=F32).astype(BF16)
    for p in range(n_pair):
        ys[p, pl.ds(pl.multiple_of(e * cap2, 16), cap2), :] = y[p * cap2:(p + 1) * cap2, :]

    @pl.when(e == local_n - 1)
    def _():
        for p in range(n_pair):
            parts = [[], [], []]
            for k in range(local_n):
                here = pick(slot_ref[p, k:k + 1, :], cap2)
                rest = gate_ref[p, k:k + 1, :]
                for part in parts:
                    head = rest.astype(BF16).astype(F32)
                    part.append(jnp.where(here, head, 0.0))
                    rest = rest - head
            total = None
            for part in parts:
                mat = jnp.concatenate(part, axis=0).astype(BF16)
                term = lax.dot_general(mat, ys[p], (((0,), (0,)), ((), ())), preferred_element_type=F32)
                total = term if total is None else total + term
            o_ref[p * width:(p + 1) * width, :] = total


def down(slot, gate, hidden, w_down, cap, start, cc):
    local_n, ff, dim = w_down.shape
    n_pair, _, width = slot.shape
    m = hidden.shape[1]
    return pl.pallas_call(
        functools.partial(down_kernel, 2 * cap),
        out_shape=jax.ShapeDtypeStruct((n_pair * width, cc), F32),
        grid=(local_n,),
        in_specs=[
            pl.BlockSpec(slot.shape, lambda e: (0, 0, 0)),
            pl.BlockSpec(gate.shape, lambda e: (0, 0, 0)),
            pl.BlockSpec(hidden.shape, lambda e: (0, 0, 0)),
            pl.BlockSpec((1, ff, cc), lambda e: (e, 0, start // cc)),
        ],
        out_specs=pl.BlockSpec((n_pair * width, cc), lambda e: (0, 0)),
        scratch_shapes=[pltpu.VMEM((n_pair, local_n * 2 * cap, cc), BF16)],
        compiler_params=pltpu.CompilerParams(vmem_limit_bytes=56 * 2 ** 20),
        cost_estimate=pl.CostEstimate(flops=2 * local_n * m * cc * ff, bytes_accessed=2 * local_n * cc * ff, transcendentals=0),
    )(slot, gate, hidden, w_down)


def solution(mesh):
    n_devs = mesh.shape['ep']

    def local_step(x_a, route_a, gate_a, h_b, attn_b, route_b, gate_b, w_qkv, w_o, w_gate, w_up, w_down):
        tok_n, dim = x_a.shape
        top_k = route_a.shape[1]
        local_n = w_gate.shape[0]
        n_experts = local_n * n_devs
        cap = min(tok_n, 2 * ((tok_n * top_k + n_experts - 1) // n_experts))
        cc = dim // 4
        small = jnp.concatenate([route_a.astype(F32), gate_a, route_b.astype(F32), gate_b], axis=1)
        small = lax.all_gather(small, 'ep')
        first = lax.axis_index('ep') * local_n
        slot_a, gw_a = slot_map(small[:, :, :top_k].astype(jnp.int32), small[:, :, top_k:2 * top_k], first, local_n, cap)
        slot_b, gw_b = slot_map(small[:, :, 2 * top_k:3 * top_k].astype(jnp.int32), small[:, :, 3 * top_k:], first, local_n, cap)

        all_a = lax.all_gather(x_a, 'ep', tiled=True)
        proj_b = jnp.dot(attn_b, w_o, preferred_element_type=F32).astype(BF16)
        mid_b = (h_b.astype(F32) + proj_b.astype(F32)).astype(BF16)
        all_b = lax.all_gather(mid_b, 'ep', tiled=True)

        def moe(tokens, everyone, slot, gw):
            hidden = gate_up(everyone, slot, w_gate, w_up, cap)
            outs = []
            for start in range(0, dim, cc):
                part = down(slot, gw, hidden, w_down, cap, start, cc)
                mix = lax.psum_scatter(part, 'ep', scatter_dimension=0, tiled=True)
                outs.append((tokens[:, start:start + cc].astype(F32) + mix).astype(BF16))
            return jnp.concatenate(outs, axis=1)

        out_a = moe(x_a, all_a, slot_a, gw_a)
        out_b = moe(mid_b, all_b, slot_b, gw_b)
        qkv_b = jnp.dot(h_b, w_qkv, preferred_element_type=F32).astype(BF16)
        return out_a, out_b, qkv_b

    row_spec = P(('dp', 'ep'), None)
    full_spec = P(None, None)
    expert_spec = P('ep', None, None)
    return jax.shard_map(
        local_step,
        mesh=mesh,
        in_specs=(row_spec, row_spec, row_spec, row_spec, row_spec, row_spec, row_spec, full_spec, full_spec, expert_spec, expert_spec, expert_spec),
        out_specs=(row_spec, row_spec, row_spec),
        check_vma=False,
    )
```

```python
import functools

import jax
import jax.numpy as jnp
from jax import lax
from jax.experimental import pallas as pl
from jax.experimental.pallas import tpu as pltpu
from jax.sharding import PartitionSpec as P

F32 = jnp.float32
BF16 = jnp.bfloat16
RING = 8
WIDE = 512


def moe_kernel(n_devs, top_k, cap, x_ref, h_ref, attn_ref, meta_ref, wqkv_ref, wo_ref, wg_ref, wu_ref, wd_ref,
               outa_ref, outb_ref, qkv_ref,
               ring, xbuf, mbuf, ubuf, rows, hidden, slots, gts, ys, p0, p1, dr, ri, fl, fr,
               ring_sem, ag_send, ag_recv, me_send, me_recv, rs_send, rs_recv, x_free, rs_free):
    tok_n, dim = x_ref.shape
    half = tok_n // 2
    local_n, _, ff = wg_ref.shape
    qkv_n = wqkv_ref.shape[1]
    cap2 = 2 * cap
    n_pair = n_devs // 2
    n_slot = local_n * cap2
    me = lax.axis_index('ep')
    core = lax.rem(me, 2)
    partner = me + 1 - 2 * core
    right = lax.rem(me + 2, n_devs)
    left = lax.rem(me + n_devs - 2, n_devs)
    first = (me * local_n).astype(F32)
    peers = (partner, left, right)

    def signal_peers(sem):
        for peer in peers:
            pl.semaphore_signal(sem, inc=1, device_id={'ep': peer}, device_id_type=pl.DeviceIdType.MESH)

    n_o, n_f, n_q, n_w = dim // WIDE, ff // WIDE, dim // WIDE, qkv_n // WIDE
    n_gu, n_d = local_n * n_f, local_n * n_q
    at_ga = n_o
    at_da = at_ga + 2 * n_gu
    at_gb = at_da + n_d
    at_db = at_gb + 2 * n_gu
    at_w = at_db + n_d
    at_end = at_w + n_w

    def cols(k):
        return pl.ds(pl.multiple_of(k * WIDE, WIDE), WIDE)

    def tall_copy(src, idx):
        slot = lax.rem(idx, RING)
        return pltpu.make_async_copy(src, ring.at[slot], ring_sem.at[slot])

    def down_copy(e, k, idx):
        slot = lax.rem(idx, RING)
        return pltpu.make_async_copy(wd_ref.at[e, :, cols(k)], ring.at[slot, pl.ds(0, ff)], ring_sem.at[slot])

    def start_gu(t, idx):
        step = t // 2
        e, f = step // n_f, step % n_f

        @pl.when(t % 2 == 0)
        def _():
            tall_copy(wg_ref.at[e, :, cols(f)], idx).start()

        @pl.when(t % 2 == 1)
        def _():
            tall_copy(wu_ref.at[e, :, cols(f)], idx).start()

    def fetch(idx, kinds):
        if 'o' in kinds:
            @pl.when(idx < at_ga)
            def _():
                tall_copy(wo_ref.at[:, cols(idx)], idx).start()
        for name, base in (('ga', at_ga), ('gb', at_gb)):
            if name in kinds:
                @pl.when((idx >= base) & (idx < base + 2 * n_gu))
                def _():
                    start_gu(idx - base, idx)
        for name, base in (('da', at_da), ('db', at_db)):
            if name in kinds:
                @pl.when((idx >= base) & (idx < base + n_d))
                def _():
                    t = idx - base
                    down_copy(t % local_n, t // local_n, idx).start()
        if 'w' in kinds:
            @pl.when((idx >= at_w) & (idx < at_end))
            def _():
                tall_copy(wqkv_ref.at[:, cols(idx - at_w)], idx).start()

    def tall(idx):
        tall_copy(wo_ref.at[:, pl.ds(0, WIDE)], idx).wait()
        return ring[lax.rem(idx, RING)]

    lo, hi = pl.ds(0, half), pl.ds(half, half)

    def ag(m, k):
        own = x_ref if m == 0 else ubuf
        src, dst, to = (
            (own.at[lo], xbuf.at[1, 0, lo], right),
            (own.at[hi], xbuf.at[1, 0, hi], right),
            (own.at[hi], xbuf.at[2, 0, hi], left),
            (own.at[lo], xbuf.at[2, 0, lo], left),
            (own, xbuf.at[0, 1], partner),
            (xbuf.at[1, 0, lo], xbuf.at[3, 0, lo], right),
            (xbuf.at[2, 0, hi], xbuf.at[3, 0, hi], left),
            (xbuf.at[1, 0], xbuf.at[1, 1], partner),
            (xbuf.at[2, 0], xbuf.at[2, 1], partner),
            (xbuf.at[3, 0, lo], xbuf.at[3, 1, lo], partner),
            (xbuf.at[3, 0, hi], xbuf.at[3, 1, hi], partner),
        )[k]
        return pltpu.make_async_remote_copy(src_ref=src, dst_ref=dst, send_sem=ag_send.at[m, k], recv_sem=ag_recv.at[m, k],
                                            device_id={'ep': to}, device_id_type=pl.DeviceIdType.MESH)

    def meta(k):
        src, dst, to = (
            (meta_ref, mbuf.at[1, 0], right),
            (meta_ref, mbuf.at[2, 0], left),
            (meta_ref, mbuf.at[0, 1], partner),
            (mbuf.at[1, 0], mbuf.at[3, 0], right),
            (mbuf.at[1, 0], mbuf.at[1, 1], partner),
            (mbuf.at[2, 0], mbuf.at[2, 1], partner),
            (mbuf.at[3, 0], mbuf.at[3, 1], partner),
        )[k]
        return pltpu.make_async_remote_copy(src_ref=src, dst_ref=dst, send_sem=me_send.at[k], recv_sem=me_recv.at[k],
                                            device_id={'ep': to}, device_id_type=pl.DeviceIdType.MESH)

    def rs(k, q):
        src, dst, to = (
            (p1.at[lax.rem(q, 2)], dr.at[q], partner),
            (p0.at[q, 3, lo], ri.at[q, 0], right),
            (p0.at[q, 3, hi], ri.at[q, 1], left),
            (p0.at[q, 2, hi], fl.at[q, hi], right),
            (p0.at[q, 1, lo], fr.at[q, lo], left),
            (p0.at[q, 2, lo], fl.at[q, lo], right),
            (p0.at[q, 1, hi], fr.at[q, hi], left),
        )[k]
        return pltpu.make_async_remote_copy(src_ref=src, dst_ref=dst, send_sem=rs_send.at[q, k], recv_sem=rs_recv.at[q, k],
                                            device_id={'ep': to}, device_id_type=pl.DeviceIdType.MESH)

    def ag_own(m):
        for k in range(5):
            ag(m, k).start()

    def ag_relay(m):
        ag(m, 0).wait_recv()
        ag(m, 5).start()
        ag(m, 2).wait_recv()
        ag(m, 6).start()

    def ag_share(m):
        ag(m, 1).wait_recv()
        ag(m, 7).start()
        ag(m, 3).wait_recv()
        ag(m, 8).start()

    def ag_share_far(m):
        ag(m, 5).wait_recv()
        ag(m, 9).start()
        ag(m, 6).wait_recv()
        ag(m, 10).start()

    lane = lax.broadcasted_iota(jnp.int32, (local_n, n_slot), 1)
    owner = lax.broadcasted_iota(jnp.int32, (local_n, n_slot), 0)
    spread = jnp.where((lane >= owner * cap2) & (lane < (owner + 1) * cap2), 1.0, 0.0).astype(F32)

    def place(m, o):
        ids = lax.broadcasted_iota(jnp.int32, (local_n, tok_n), 0).astype(F32) + first
        tri = jnp.where(lax.broadcasted_iota(jnp.int32, (tok_n, tok_n), 0) < lax.broadcasted_iota(jnp.int32, (tok_n, tok_n), 1),
                        1.0, 0.0).astype(BF16)
        slot_parts, gate_parts = [], []
        for j in range(2):
            member = jnp.zeros((local_n, tok_n), F32)
            gate = jnp.zeros((local_n, tok_n), F32)
            for t in range(top_k):
                hit = mbuf[o, j, 16 * m + t:16 * m + t + 1, :] == ids
                member = jnp.where(hit, 1.0, member)
                gate = jnp.where(hit, mbuf[o, j, 16 * m + 8 + t:16 * m + 9 + t, :], gate)
            rank = jnp.dot(member.astype(BF16), tri, preferred_element_type=F32)
            slot_parts.append(jnp.where(member > 0.5, rank + float(j * cap), -1.0))
            gate_parts.append(gate)
        slot = jnp.concatenate(slot_parts, axis=1)
        gate = jnp.concatenate(gate_parts, axis=1)
        slots[...] = slot
        index = lax.broadcasted_iota(jnp.int32, (cap2, 2 * tok_n), 0).astype(F32)
        sel = jnp.concatenate([jnp.where(index == slots[e:e + 1, :], 1.0, 0.0) for e in range(local_n)], axis=0).astype(BF16)
        wide = 2 * WIDE
        both = xbuf[o].reshape(2 * tok_n, dim)
        for k in range(0, dim, wide):
            n = min(wide, dim - k)
            got = jnp.dot(sel, both[:, k:k + n], preferred_element_type=F32).astype(BF16)
            for e in range(local_n):
                rows[e, o * cap2:(o + 1) * cap2, k:k + n] = got[e * cap2:(e + 1) * cap2, :]

        def over(a):
            return lax.dot_general(a, spread, (((0,), (0,)), ((), ())), preferred_element_type=F32)

        pos = lax.broadcasted_iota(jnp.int32, (2 * tok_n, n_slot), 1)
        pos = lax.rem(pos, cap2).astype(F32)
        here = over(slot) == pos
        rest = gate
        for part in range(3):
            head = rest.astype(BF16).astype(F32)
            gts[o, part] = jnp.where(here, over(head), 0.0).astype(BF16)
            rest = rest - head

    def gate_up(base, kinds, events):
        def step(i, carry):
            at = base + 2 * i
            e, f = i // n_f, i % n_f
            tall_copy(wo_ref.at[:, pl.ds(0, WIDE)], at).wait()
            tall_copy(wo_ref.at[:, pl.ds(0, WIDE)], at + 1).wait()
            mine = rows[e]
            gate = jnp.dot(mine, ring[lax.rem(at, RING)], preferred_element_type=F32)
            up = jnp.dot(mine, ring[lax.rem(at + 1, RING)], preferred_element_type=F32)
            hidden[e, :, cols(f)] = (jax.nn.silu(gate) * up).astype(BF16)
            fetch(at + RING, kinds)
            fetch(at + 1 + RING, kinds)
            for when, event in events:
                @pl.when(i == when)
                def _():
                    event()
            return carry

        lax.fori_loop(0, n_gu, step, 0)

    def stage1(q):
        rs(0, q).wait_recv()
        for o in (3, 2, 1, 0):
            p0[q, o] = p0[q, o] + dr[q, o]
        for k in (1, 2, 3, 4):
            rs(k, q).start()

    def stage2(q):
        rs(1, q).wait_recv()
        rs(2, q).wait_recv()
        p0[q, 2, lo] = p0[q, 2, lo] + ri[q, 0]
        p0[q, 1, hi] = p0[q, 1, hi] + ri[q, 1]
        rs(5, q).start()
        rs(6, q).start()

    def combine(q):
        for o in range(n_pair):
            total = None
            for part in range(3):
                term = jnp.dot(gts[o, part], ys[o], preferred_element_type=F32)
                total = term if total is None else total + term
            p1[lax.rem(q, 2), o] = total[tok_n:, :]
            p0[q, o] = total[:tok_n, :]

    def down(m, base, kinds):
        def step(i, carry):
            at = base + i
            q, e = i // local_n, i % local_n
            down_copy(0, 0, at).wait()
            y = jnp.dot(hidden[e], ring[lax.rem(at, RING), pl.ds(0, ff)], preferred_element_type=F32).astype(BF16)
            for o in range(n_pair):
                ys[o, pl.ds(pl.multiple_of(e * cap2, 16), cap2), :] = y[o * cap2:(o + 1) * cap2, :]
            fetch(at + RING, kinds)

            @pl.when((e == 4) & (q >= 1))
            def _():
                stage1(q - 1)

            @pl.when((e == 1) & (q >= 2))
            def _():
                stage2(q - 2)

            @pl.when(e == local_n - 1)
            def _():
                @pl.when(q >= 2)
                def _():
                    rs(0, q - 2).wait_send()
                combine(q)
                if m == 1:
                    @pl.when(q == 0)
                    def _():
                        pl.semaphore_wait(rs_free, len(peers))
                rs(0, q).start()
            return carry

        lax.fori_loop(0, n_d, step, 0)

    def finish(m):
        tokens, out = (x_ref, outa_ref) if m == 0 else (ubuf, outb_ref)

        def step(q, carry):
            for k in (3, 4, 5, 6):
                rs(k, q).wait_recv()
            total = p0[q, 0] + fl[q] + fr[q]
            out[:, cols(q)] = (tokens[:, cols(q)].astype(F32) + total).astype(BF16)
            return carry

        lax.fori_loop(0, n_q, step, 0)

        def drain(q, carry):
            for k in (1, 2, 3, 4, 5, 6):
                rs(k, q).wait_send()
            return carry

        lax.fori_loop(0, n_q, drain, 0)
        for q in (n_q - 2, n_q - 1):
            rs(0, q).wait_send()

    for idx in range(RING):
        fetch(idx, ('o', 'ga'))
    barrier = pltpu.get_barrier_semaphore()
    signal_peers(barrier)
    pl.semaphore_wait(barrier, len(peers))
    for k in (0, 1, 2):
        meta(k).start()
    ag_own(0)
    mbuf[0, 0] = meta_ref[...]
    xbuf[0, 0] = x_ref[...]

    def project(i, carry):
        proj = jnp.dot(attn_ref[...], tall(i), preferred_element_type=F32).astype(BF16)
        ubuf[:, cols(i)] = (h_ref[:, cols(i)].astype(F32) + proj.astype(F32)).astype(BF16)
        fetch(i + RING, ('ga',))
        return carry

    lax.fori_loop(0, n_o, project, 0)
    meta(0).wait_recv()
    meta(3).start()
    meta(4).start()
    meta(1).wait_recv()
    meta(5).start()
    meta(2).wait_recv()
    ag(0, 4).wait_recv()
    place(0, 0)
    ag_relay(0)
    meta(3).wait_recv()
    meta(6).start()
    for k in (4, 5, 6):
        meta(k).wait_recv()
    ag_share(0)
    ag(0, 7).wait_recv()
    place(0, 1)
    ag(0, 8).wait_recv()
    place(0, 2)
    ag_share_far(0)
    ag(0, 9).wait_recv()
    ag(0, 10).wait_recv()
    place(0, 3)
    for k in range(11):
        ag(0, k).wait_send()
    for k in range(7):
        meta(k).wait_send()
    signal_peers(x_free)

    def send_b():
        pl.semaphore_wait(x_free, len(peers))
        ag_own(1)
        xbuf[0, 0] = ubuf[...]

    gate_up(at_ga, ('ga', 'da'), (
        (1, send_b),
        (8, lambda: ag_relay(1)),
        (13, lambda: ag_share(1)),
        (18, lambda: ag_share_far(1)),
    ))
    down(0, at_da, ('da', 'gb'))
    for k in (4, 7, 8, 9, 10):
        ag(1, k).wait_recv()
    for o in range(n_pair):
        place(1, o)
        if o == 1:
            stage1(n_q - 1)
    gate_up(at_gb, ('gb', 'db'), (
        (1, lambda: stage2(n_q - 2)),
        (5, lambda: stage2(n_q - 1)),
    ))
    finish(0)
    signal_peers(rs_free)
    down(1, at_db, ('db', 'w'))

    def qkv(i, carry):
        qkv_ref[:, cols(i)] = jnp.dot(h_ref[...], tall(at_w + i), preferred_element_type=F32).astype(BF16)

        @pl.when(i == 2)
        def _():
            stage1(n_q - 1)

        @pl.when(i == 3)
        def _():
            stage2(n_q - 2)
        return carry

    lax.fori_loop(0, n_w, qkv, 0)
    stage2(n_q - 1)
    finish(1)
    for k in range(11):
        ag(1, k).wait_send()


def solution(mesh):
    n_devs = mesh.shape['ep']

    def local_step(x_a, route_a, gate_a, h_b, attn_b, route_b, gate_b, w_qkv, w_o, w_gate, w_up, w_down):
        tok_n, dim = x_a.shape
        top_k = route_a.shape[1]
        local_n, _, ff = w_gate.shape
        qkv_n = w_qkv.shape[1]
        n_experts = local_n * n_devs
        cap = min(tok_n, 2 * ((tok_n * top_k + n_experts - 1) // n_experts))
        n_pair = n_devs // 2
        n_q = dim // WIDE
        cap2 = 2 * cap
        m = n_pair * cap2
        half = tok_n // 2

        def eight(a):
            return jnp.concatenate([a.astype(F32).T, jnp.full((8 - top_k, tok_n), -1.0, F32)], axis=0)

        meta = jnp.concatenate([eight(route_a), eight(gate_a), eight(route_b), eight(gate_b)], axis=0)
        vmem = pl.BlockSpec(memory_space=pltpu.VMEM)
        hbm = pl.BlockSpec(memory_space=pl.ANY)
        flops = 2 * 2 * 3 * local_n * m * dim * ff
        weight_bytes = 2 * 6 * local_n * dim * ff
        return pl.pallas_call(
            functools.partial(moe_kernel, n_devs, top_k, cap),
            out_shape=(
                jax.ShapeDtypeStruct((tok_n, dim), BF16),
                jax.ShapeDtypeStruct((tok_n, dim), BF16),
                jax.ShapeDtypeStruct((tok_n, qkv_n), BF16),
            ),
            in_specs=[vmem] * 4 + [hbm] * 5,
            out_specs=(vmem, vmem, vmem),
            scratch_shapes=[
                pltpu.VMEM((RING, dim, WIDE), BF16),
                pltpu.VMEM((n_pair, 2, tok_n, dim), BF16),
                pltpu.VMEM((n_pair, 2, 32, tok_n), F32),
                pltpu.VMEM((tok_n, dim), BF16),
                pltpu.VMEM((local_n, m, dim), BF16),
                pltpu.VMEM((local_n, m, ff), BF16),
                pltpu.VMEM((local_n, 2 * tok_n), F32),
                pltpu.VMEM((n_pair, 3, 2 * tok_n, local_n * cap2), BF16),
                pltpu.VMEM((n_pair, local_n * cap2, WIDE), BF16),
                pltpu.VMEM((n_q, n_pair, tok_n, WIDE), F32),
                pltpu.VMEM((2, n_pair, tok_n, WIDE), F32),
                pltpu.VMEM((n_q, n_pair, tok_n, WIDE), F32),
                pltpu.VMEM((n_q, 2, half, WIDE), F32),
                pltpu.VMEM((n_q, tok_n, WIDE), F32),
                pltpu.VMEM((n_q, tok_n, WIDE), F32),
                pltpu.SemaphoreType.DMA((RING,)),
                pltpu.SemaphoreType.DMA((2, 11)),
                pltpu.SemaphoreType.DMA((2, 11)),
                pltpu.SemaphoreType.DMA((7,)),
                pltpu.SemaphoreType.DMA((7,)),
                pltpu.SemaphoreType.DMA((n_q, 7)),
                pltpu.SemaphoreType.DMA((n_q, 7)),
                pltpu.SemaphoreType.REGULAR,
                pltpu.SemaphoreType.REGULAR,
            ],
            compiler_params=pltpu.CompilerParams(collective_id=0, has_side_effects=True, vmem_limit_bytes=67043328),
            cost_estimate=pl.CostEstimate(flops=flops, bytes_accessed=weight_bytes, transcendentals=0),
        )(x_a, h_b, attn_b, meta, w_qkv, w_o, w_gate, w_up, w_down)

    row_spec = P(('dp', 'ep'), None)
    full_spec = P(None, None)
    expert_spec = P('ep', None, None)
    return jax.shard_map(
        local_step,
        mesh=mesh,
        in_specs=(row_spec, row_spec, row_spec, row_spec, row_spec, row_spec, row_spec, full_spec, full_spec, expert_spec, expert_spec, expert_spec),
        out_specs=(row_spec, row_spec, row_spec),
        check_vma=False,
    )
```

```python
import functools

import jax
import jax.numpy as jnp
from jax import lax
from jax.experimental import pallas as pl
from jax.experimental.pallas import tpu as pltpu
from jax.sharding import PartitionSpec as P

F32 = jnp.float32
BF16 = jnp.bfloat16
RING = 8
WIDE = 512


def moe_kernel(n_devs, top_k, cap, x_ref, h_ref, attn_ref, ra_ref, ga_ref, rb_ref, gb_ref, wqkv_ref, wo_ref, wg_ref, wu_ref, wd_ref,
               outa_ref, outb_ref, qkv_ref,
               ring, xbuf, mbuf, ubuf, rows, hidden, slots, gts, ys, p0, p1, dr, ri, fl, fr,
               ring_sem, ag_send, ag_recv, me_send, me_recv, rs_send, rs_recv, x_free, rs_free):
    tok_n, dim = x_ref.shape
    half = tok_n // 2
    local_n, _, ff = wg_ref.shape
    qkv_n = wqkv_ref.shape[1]
    cap2 = 2 * cap
    n_pair = n_devs // 2
    n_slot = local_n * cap
    me = lax.axis_index('ep')
    core = lax.rem(me, 2)
    partner = me + 1 - 2 * core
    right = lax.rem(me + 2, n_devs)
    left = lax.rem(me + n_devs - 2, n_devs)
    first = (me * local_n).astype(F32)
    peers = (partner, left, right)

    def signal_peers(sem):
        for peer in peers:
            pl.semaphore_signal(sem, inc=1, device_id={'ep': peer}, device_id_type=pl.DeviceIdType.MESH)

    n_o, n_f, n_q, n_w = dim // WIDE, ff // WIDE, dim // WIDE, qkv_n // WIDE
    n_gu, n_d = local_n * n_f, local_n * n_q
    at_ga = n_o
    at_da = at_ga + 2 * n_gu
    at_gb = at_da + n_d
    at_db = at_gb + 2 * n_gu
    at_w = at_db + n_d
    at_end = at_w + n_w

    def cols(k):
        return pl.ds(pl.multiple_of(k * WIDE, WIDE), WIDE)

    def tall_copy(src, idx):
        slot = lax.rem(idx, RING)
        return pltpu.make_async_copy(src, ring.at[slot], ring_sem.at[slot])

    def down_copy(e, k, idx):
        slot = lax.rem(idx, RING)
        return pltpu.make_async_copy(wd_ref.at[e, :, cols(k)], ring.at[slot, pl.ds(0, ff)], ring_sem.at[slot])

    def start_gu(t, idx):
        step = t // 2
        e, f = step // n_f, step % n_f

        @pl.when(t % 2 == 0)
        def _():
            tall_copy(wg_ref.at[e, :, cols(f)], idx).start()

        @pl.when(t % 2 == 1)
        def _():
            tall_copy(wu_ref.at[e, :, cols(f)], idx).start()

    def fetch(idx, kinds):
        if 'o' in kinds:
            @pl.when(idx < at_ga)
            def _():
                tall_copy(wo_ref.at[:, cols(idx)], idx).start()
        for name, base in (('ga', at_ga), ('gb', at_gb)):
            if name in kinds:
                @pl.when((idx >= base) & (idx < base + 2 * n_gu))
                def _():
                    start_gu(idx - base, idx)
        for name, base in (('da', at_da), ('db', at_db)):
            if name in kinds:
                @pl.when((idx >= base) & (idx < base + n_d))
                def _():
                    t = idx - base
                    down_copy(t % local_n, t // local_n, idx).start()
        if 'w' in kinds:
            @pl.when((idx >= at_w) & (idx < at_end))
            def _():
                tall_copy(wqkv_ref.at[:, cols(idx - at_w)], idx).start()

    def tall(idx):
        tall_copy(wo_ref.at[:, pl.ds(0, WIDE)], idx).wait()
        return ring[lax.rem(idx, RING)]

    lo, hi = pl.ds(0, half), pl.ds(half, half)

    def ag(m, k):
        own = x_ref if m == 0 else ubuf
        src, dst, to = (
            (own.at[lo], xbuf.at[1, 0, lo], right),
            (own.at[hi], xbuf.at[1, 0, hi], right),
            (own.at[hi], xbuf.at[2, 0, hi], left),
            (own.at[lo], xbuf.at[2, 0, lo], left),
            (own, xbuf.at[0, 1], partner),
            (xbuf.at[1, 0, lo], xbuf.at[3, 0, lo], right),
            (xbuf.at[2, 0, hi], xbuf.at[3, 0, hi], left),
            (xbuf.at[1, 0], xbuf.at[1, 1], partner),
            (xbuf.at[2, 0], xbuf.at[2, 1], partner),
            (xbuf.at[3, 0, lo], xbuf.at[3, 1, lo], partner),
            (xbuf.at[3, 0, hi], xbuf.at[3, 1, hi], partner),
        )[k]
        return pltpu.make_async_remote_copy(src_ref=src, dst_ref=dst, send_sem=ag_send.at[m, k], recv_sem=ag_recv.at[m, k],
                                            device_id={'ep': to}, device_id_type=pl.DeviceIdType.MESH)

    def meta(k):
        src, dst, to = (
            (mbuf.at[0, 0], mbuf.at[1, 0], right),
            (mbuf.at[0, 0], mbuf.at[2, 0], left),
            (mbuf.at[0, 0], mbuf.at[0, 1], partner),
            (mbuf.at[1, 0], mbuf.at[3, 0], right),
            (mbuf.at[1, 0], mbuf.at[1, 1], partner),
            (mbuf.at[2, 0], mbuf.at[2, 1], partner),
            (mbuf.at[3, 0], mbuf.at[3, 1], partner),
        )[k]
        return pltpu.make_async_remote_copy(src_ref=src, dst_ref=dst, send_sem=me_send.at[k], recv_sem=me_recv.at[k],
                                            device_id={'ep': to}, device_id_type=pl.DeviceIdType.MESH)

    def rs(k, q):
        src, dst, to = (
            (p1.at[lax.rem(q, 2)], dr.at[q], partner),
            (p0.at[q, 3, lo], ri.at[q, 0], right),
            (p0.at[q, 3, hi], ri.at[q, 1], left),
            (p0.at[q, 2, hi], fl.at[q, hi], right),
            (p0.at[q, 1, lo], fr.at[q, lo], left),
            (p0.at[q, 2, lo], fl.at[q, lo], right),
            (p0.at[q, 1, hi], fr.at[q, hi], left),
        )[k]
        return pltpu.make_async_remote_copy(src_ref=src, dst_ref=dst, send_sem=rs_send.at[q, k], recv_sem=rs_recv.at[q, k],
                                            device_id={'ep': to}, device_id_type=pl.DeviceIdType.MESH)

    def ag_own(m):
        for k in range(5):
            ag(m, k).start()

    def ag_relay(m):
        ag(m, 0).wait_recv()
        ag(m, 5).start()
        ag(m, 2).wait_recv()
        ag(m, 6).start()

    def ag_share(m):
        ag(m, 1).wait_recv()
        ag(m, 7).start()
        ag(m, 3).wait_recv()
        ag(m, 8).start()

    def ag_share_far(m):
        ag(m, 5).wait_recv()
        ag(m, 9).start()
        ag(m, 6).wait_recv()
        ag(m, 10).start()

    lane = lax.broadcasted_iota(jnp.int32, (local_n, n_slot), 1)
    owner = lax.broadcasted_iota(jnp.int32, (local_n, n_slot), 0)
    spread = jnp.where((lane >= owner * cap) & (lane < (owner + 1) * cap), 1.0, 0.0).astype(F32)

    def place(m, o):
        ids = lax.broadcasted_iota(jnp.int32, (local_n, tok_n), 0).astype(F32) + first
        tri = jnp.where(lax.broadcasted_iota(jnp.int32, (tok_n, tok_n), 0) < lax.broadcasted_iota(jnp.int32, (tok_n, tok_n), 1),
                        1.0, 0.0).astype(BF16)
        pos = lax.rem(lax.broadcasted_iota(jnp.int32, (tok_n, n_slot), 1), cap).astype(F32)

        def over(a):
            return lax.dot_general(a, spread, (((0,), (0,)), ((), ())), preferred_element_type=F32)

        for j in range(2):
            member = jnp.zeros((local_n, tok_n), F32)
            gate = jnp.zeros((local_n, tok_n), F32)
            for t in range(top_k):
                hit = mbuf[o, j, 16 * m + t:16 * m + t + 1, :] == ids
                member = jnp.where(hit, 1.0, member)
                gate = jnp.where(hit, mbuf[o, j, 16 * m + 8 + t:16 * m + 9 + t, :], gate)
            rank = jnp.dot(member.astype(BF16), tri, preferred_element_type=F32)
            slots[:, j * tok_n:(j + 1) * tok_n] = jnp.where(member > 0.5, rank + float(j * cap), -1.0)
            here = over(jnp.where(member > 0.5, rank, -1.0)) == pos
            rest = gate
            for part in range(3):
                head = rest.astype(BF16).astype(F32)
                gts[o, j, part] = jnp.where(here, over(head), 0.0).astype(BF16)
                rest = rest - head
        index = lax.broadcasted_iota(jnp.int32, (cap2, 2 * tok_n), 0).astype(F32)
        sel = jnp.concatenate([jnp.where(index == slots[e:e + 1, :], 1.0, 0.0) for e in range(local_n)], axis=0).astype(BF16)
        wide = 2 * WIDE
        both = xbuf[o].reshape(2 * tok_n, dim)
        for k in range(0, dim, wide):
            n = min(wide, dim - k)
            got = jnp.dot(sel, both[:, k:k + n], preferred_element_type=F32).astype(BF16)
            for e in range(local_n):
                rows[e, o * cap2:(o + 1) * cap2, k:k + n] = got[e * cap2:(e + 1) * cap2, :]

    def gate_up(base, kinds, events):
        def step(i, carry):
            at = base + 2 * i
            e, f = i // n_f, i % n_f
            tall_copy(wo_ref.at[:, pl.ds(0, WIDE)], at).wait()
            tall_copy(wo_ref.at[:, pl.ds(0, WIDE)], at + 1).wait()
            mine = rows[e]
            gate = jnp.dot(mine, ring[lax.rem(at, RING)], preferred_element_type=F32)
            up = jnp.dot(mine, ring[lax.rem(at + 1, RING)], preferred_element_type=F32)
            hidden[e, :, cols(f)] = (jax.nn.silu(gate) * up).astype(BF16)
            fetch(at + RING, kinds)
            fetch(at + 1 + RING, kinds)
            events(i)
            return carry

        lax.fori_loop(0, n_gu, step, 0)

    def stage1(q):
        rs(0, q).wait_recv()
        for o in (3, 2, 1, 0):
            p0[q, o] = p0[q, o] + dr[q, o]
        for k in (1, 2, 3, 4):
            rs(k, q).start()

    def stage2(q):
        rs(1, q).wait_recv()
        rs(2, q).wait_recv()
        p0[q, 2, lo] = p0[q, 2, lo] + ri[q, 0]
        p0[q, 1, hi] = p0[q, 1, hi] + ri[q, 1]
        rs(5, q).start()
        rs(6, q).start()

    def combine(q):
        for o in range(n_pair):
            for j in (1, 0):
                total = None
                for part in range(3):
                    term = jnp.dot(gts[o, j, part], ys[o, j], preferred_element_type=F32)
                    total = term if total is None else total + term
                if j == 1:
                    p1[lax.rem(q, 2), o] = total
                else:
                    p0[q, o] = total

    def down(m, base, kinds):
        n_e = local_n // 2

        def step(i, carry):
            at = base + 2 * i
            q, e = i // n_e, i % n_e
            down_copy(0, 0, at).wait()
            down_copy(0, 0, at + 1).wait()
            y0 = jnp.dot(hidden[2 * e], ring[lax.rem(at, RING), pl.ds(0, ff)], preferred_element_type=F32)
            y1 = jnp.dot(hidden[2 * e + 1], ring[lax.rem(at + 1, RING), pl.ds(0, ff)], preferred_element_type=F32)
            for o in range(n_pair):
                for j in range(2):
                    here = slice(o * cap2 + j * cap, o * cap2 + (j + 1) * cap)
                    two = jnp.concatenate([y0[here], y1[here]], axis=0)
                    ys[o, j, pl.ds(pl.multiple_of(e * cap2, 16), cap2), :] = two.astype(BF16)
            fetch(at + RING, kinds)
            fetch(at + 1 + RING, kinds)

            @pl.when((e == 1) & (q >= 1))
            def _():
                stage1(q - 1)

            @pl.when(e == n_e - 1)
            def _():
                @pl.when(q >= 2)
                def _():
                    rs(0, q - 2).wait_send()
                combine(q)
                if m == 1:
                    @pl.when(q == 0)
                    def _():
                        pl.semaphore_wait(rs_free, len(peers))
                rs(0, q).start()
            return carry

        lax.fori_loop(0, n_d // 2, step, 0)

    def finish(m):
        tokens, out = (x_ref, outa_ref) if m == 0 else (ubuf, outb_ref)

        def step(q, carry):
            for k in (3, 4, 5, 6):
                rs(k, q).wait_recv()
            total = p0[q, 0] + fl[q] + fr[q]
            out[:, cols(q)] = (tokens[:, cols(q)].astype(F32) + total).astype(BF16)
            return carry

        lax.fori_loop(0, n_q, step, 0)

        def drain(q, carry):
            for k in (1, 2, 3, 4, 5, 6):
                rs(k, q).wait_send()
            return carry

        lax.fori_loop(0, n_q, drain, 0)
        for q in (n_q - 2, n_q - 1):
            rs(0, q).wait_send()

    for idx in range(RING):
        fetch(idx, ('o', 'ga'))
    barrier = pltpu.get_barrier_semaphore()
    signal_peers(barrier)
    mbuf[0, 0] = jnp.zeros_like(mbuf[0, 0])
    for at, ref in ((0, ra_ref), (8, ga_ref), (16, rb_ref), (24, gb_ref)):
        mbuf[0, 0, at:at + top_k, :] = ref[...].astype(F32)
    pl.semaphore_wait(barrier, len(peers))
    for k in (0, 1, 2):
        meta(k).start()
    ag_own(0)
    xbuf[0, 0] = x_ref[...]

    def project(i, carry):
        proj = jnp.dot(attn_ref[...], tall(i), preferred_element_type=F32).astype(BF16)
        ubuf[:, cols(i)] = (h_ref[:, cols(i)].astype(F32) + proj.astype(F32)).astype(BF16)
        fetch(i + RING, ('ga',))
        return carry

    lax.fori_loop(0, n_o, project, 0)
    meta(0).wait_recv()
    meta(3).start()
    meta(4).start()
    meta(1).wait_recv()
    meta(5).start()
    meta(2).wait_recv()
    ag(0, 4).wait_recv()
    place(0, 0)
    ag_relay(0)
    meta(3).wait_recv()
    meta(6).start()
    for k in (4, 5, 6):
        meta(k).wait_recv()
    ag_share(0)
    ag(0, 7).wait_recv()
    place(0, 1)
    ag(0, 8).wait_recv()
    place(0, 2)
    ag_share_far(0)
    ag(0, 9).wait_recv()
    ag(0, 10).wait_recv()
    place(0, 3)
    for k in range(11):
        ag(0, k).wait_send()
    for k in range(7):
        meta(k).wait_send()
    signal_peers(x_free)

    def send_b():
        pl.semaphore_wait(x_free, len(peers))
        ag_own(1)
        xbuf[0, 0] = ubuf[...]

    def during_a(i):
        for when, event in ((1, send_b), (8, lambda: ag_relay(1)), (13, lambda: ag_share(1)), (18, lambda: ag_share_far(1))):
            @pl.when(i == when)
            def _():
                event()

    gate_up(at_ga, ('ga', 'da'), during_a)
    down(0, at_da, ('da', 'gb'))
    for k in (4, 7, 8, 9, 10):
        ag(1, k).wait_recv()
    for o in range(n_pair):
        place(1, o)
        if o == 1:
            stage1(n_q - 1)

    def during_b(i):
        @pl.when((i % 2 == 1) & (i < 2 * n_q))
        def _():
            stage2(i // 2)

    gate_up(at_gb, ('gb', 'db'), during_b)
    finish(0)
    signal_peers(rs_free)
    down(1, at_db, ('db', 'w'))

    def qkv(i, carry):
        qkv_ref[:, cols(i)] = jnp.dot(h_ref[...], tall(at_w + i), preferred_element_type=F32).astype(BF16)

        @pl.when(i == 1)
        def _():
            stage1(n_q - 1)

        @pl.when((i >= 2) & (i - 2 < n_q - 1))
        def _():
            stage2(i - 2)
        return carry

    lax.fori_loop(0, n_w, qkv, 0)
    stage2(n_q - 1)
    finish(1)
    for k in range(11):
        ag(1, k).wait_send()


def write_kernel(a_ref, b_ref, c_ref, oa_ref, ob_ref, oc_ref, va, vb, vc, sem_in, sem_out):
    moves = ((a_ref, va, oa_ref), (b_ref, vb, ob_ref), (c_ref, vc, oc_ref))
    for k, (src, buf, _) in enumerate(moves):
        pltpu.make_async_copy(src, buf, sem_in.at[k]).start()
    for k, (src, buf, dst) in enumerate(moves):
        pltpu.make_async_copy(src, buf, sem_in.at[k]).wait()
        pltpu.make_async_copy(buf, dst, sem_out.at[k]).start()
    for k, (_, buf, dst) in enumerate(moves):
        pltpu.make_async_copy(buf, dst, sem_out.at[k]).wait()


def write_out(arrays):
    hbm = pl.BlockSpec(memory_space=pl.ANY)
    return pl.pallas_call(
        write_kernel,
        out_shape=tuple(jax.ShapeDtypeStruct(a.shape, a.dtype) for a in arrays),
        in_specs=[hbm] * 3,
        out_specs=(hbm,) * 3,
        scratch_shapes=[pltpu.VMEM(a.shape, a.dtype) for a in arrays] + [pltpu.SemaphoreType.DMA((3,)), pltpu.SemaphoreType.DMA((3,))],
    )(*arrays)


def solution(mesh):
    n_devs = mesh.shape['ep']

    def local_step(x_a, route_a, gate_a, h_b, attn_b, route_b, gate_b, w_qkv, w_o, w_gate, w_up, w_down):
        tok_n, dim = x_a.shape
        top_k = route_a.shape[1]
        local_n, _, ff = w_gate.shape
        qkv_n = w_qkv.shape[1]
        n_experts = local_n * n_devs
        cap = min(tok_n, 2 * ((tok_n * top_k + n_experts - 1) // n_experts))
        n_pair = n_devs // 2
        n_q = dim // WIDE
        cap2 = 2 * cap
        m = n_pair * cap2
        half = tok_n // 2

        vmem = pl.BlockSpec(memory_space=pltpu.VMEM)
        hbm = pl.BlockSpec(memory_space=pl.ANY)
        flops = 2 * 2 * 3 * local_n * m * dim * ff
        weight_bytes = 2 * 6 * local_n * dim * ff
        results = pl.pallas_call(
            functools.partial(moe_kernel, n_devs, top_k, cap),
            out_shape=(
                jax.ShapeDtypeStruct((tok_n, dim), BF16),
                jax.ShapeDtypeStruct((tok_n, dim), BF16),
                jax.ShapeDtypeStruct((tok_n, qkv_n), BF16),
            ),
            in_specs=[vmem] * 7 + [hbm] * 5,
            out_specs=(vmem, vmem, vmem),
            scratch_shapes=[
                pltpu.VMEM((RING, dim, WIDE), BF16),
                pltpu.VMEM((n_pair, 2, tok_n, dim), BF16),
                pltpu.VMEM((n_pair, 2, 32, tok_n), F32),
                pltpu.VMEM((tok_n, dim), BF16),
                pltpu.VMEM((local_n, m, dim), BF16),
                pltpu.VMEM((local_n, m, ff), BF16),
                pltpu.VMEM((local_n, 2 * tok_n), F32),
                pltpu.VMEM((n_pair, 2, 3, tok_n, local_n * cap), BF16),
                pltpu.VMEM((n_pair, 2, local_n * cap, WIDE), BF16),
                pltpu.VMEM((n_q, n_pair, tok_n, WIDE), F32),
                pltpu.VMEM((2, n_pair, tok_n, WIDE), F32),
                pltpu.VMEM((n_q, n_pair, tok_n, WIDE), F32),
                pltpu.VMEM((n_q, 2, half, WIDE), F32),
                pltpu.VMEM((n_q, tok_n, WIDE), F32),
                pltpu.VMEM((n_q, tok_n, WIDE), F32),
                pltpu.SemaphoreType.DMA((RING,)),
                pltpu.SemaphoreType.DMA((2, 11)),
                pltpu.SemaphoreType.DMA((2, 11)),
                pltpu.SemaphoreType.DMA((7,)),
                pltpu.SemaphoreType.DMA((7,)),
                pltpu.SemaphoreType.DMA((n_q, 7)),
                pltpu.SemaphoreType.DMA((n_q, 7)),
                pltpu.SemaphoreType.REGULAR,
                pltpu.SemaphoreType.REGULAR,
            ],
            compiler_params=pltpu.CompilerParams(collective_id=0, has_side_effects=True, vmem_limit_bytes=67043328),
            cost_estimate=pl.CostEstimate(flops=flops, bytes_accessed=weight_bytes, transcendentals=0),
        )(x_a, h_b, attn_b, route_a.T, gate_a.T, route_b.T, gate_b.T, w_qkv, w_o, w_gate, w_up, w_down)
        return write_out(results)

    row_spec = P(('dp', 'ep'), None)
    full_spec = P(None, None)
    expert_spec = P('ep', None, None)
    return jax.shard_map(
        local_step,
        mesh=mesh,
        in_specs=(row_spec, row_spec, row_spec, row_spec, row_spec, row_spec, row_spec, full_spec, full_spec, expert_spec, expert_spec, expert_spec),
        out_specs=(row_spec, row_spec, row_spec),
        check_vma=False,
    )
```

```python
import functools

import jax
import jax.numpy as jnp
from jax import lax
from jax.experimental import pallas as pl
from jax.experimental.pallas import tpu as pltpu
from jax.sharding import PartitionSpec as P

F32 = jnp.float32
BF16 = jnp.bfloat16
RING = 8
WIDE = 512
SHARED = 2


def moe_kernel(n_devs, top_k, cap, ra_ref, ga_ref, rb_ref, gb_ref, x_ref, h_ref, attn_ref,
               wqkv_ref, wo_ref, wg_ref, wu_ref, wd_ref,
               outa_ref, outb_ref, qkv_ref,
               ring, xbuf, mbuf, ubuf, abuf, bbuf, hbuf, qbuf, rows, hidden, later, slots, gts, ys, p0, p1, dr, ri, fl, fr,
               ring_sem, io_sem, ag_send, ag_recv, me_send, me_recv, rs_send, rs_recv, x_free, rs_free):
    tok_n, dim = x_ref.shape
    half = tok_n // 2
    local_n, _, ff = wg_ref.shape
    qkv_n = wqkv_ref.shape[1]
    cap2 = 2 * cap
    n_pair = n_devs // 2
    n_slot = local_n * cap
    me = lax.axis_index('ep')
    core = lax.rem(me, 2)
    partner = me + 1 - 2 * core
    right = lax.rem(me + 2, n_devs)
    left = lax.rem(me + n_devs - 2, n_devs)
    first = (me * local_n).astype(F32)
    peers = (partner, left, right)

    def signal_peers(sem):
        for peer in peers:
            pl.semaphore_signal(sem, inc=1, device_id={'ep': peer}, device_id_type=pl.DeviceIdType.MESH)

    n_o, n_f, n_q, n_w = dim // WIDE, ff // WIDE, dim // WIDE, qkv_n // WIDE
    n_ga, n_gb, n_d = local_n * n_f, (local_n - SHARED) * n_f, local_n * n_q
    at_ga = n_o
    at_da = at_ga + 2 * n_ga
    at_gb = at_da + n_d
    at_db = at_gb + 2 * n_gb
    at_w = at_db + n_d
    at_end = at_w + n_w

    def cols(k):
        return pl.ds(pl.multiple_of(k * WIDE, WIDE), WIDE)

    def tall_copy(src, idx):
        slot = lax.rem(idx, RING)
        return pltpu.make_async_copy(src, ring.at[slot], ring_sem.at[slot])

    def down_copy(e, k, idx):
        slot = lax.rem(idx, RING)
        return pltpu.make_async_copy(wd_ref.at[e, :, cols(k)], ring.at[slot, pl.ds(0, ff)], ring_sem.at[slot])

    def start_gu(t, idx):
        step = t // 2
        e, f = step // n_f, step % n_f

        @pl.when(t % 2 == 0)
        def _():
            tall_copy(wg_ref.at[e, :, cols(f)], idx).start()

        @pl.when(t % 2 == 1)
        def _():
            tall_copy(wu_ref.at[e, :, cols(f)], idx).start()

    def fetch(idx, kinds):
        if 'o' in kinds:
            @pl.when(idx < at_ga)
            def _():
                tall_copy(wo_ref.at[:, cols(idx)], idx).start()
        for name, base, steps in (('ga', at_ga, n_ga), ('gb', at_gb, n_gb)):
            if name in kinds:
                @pl.when((idx >= base) & (idx < base + 2 * steps))
                def _():
                    start_gu(idx - base, idx)
        for name, base in (('da', at_da), ('db', at_db)):
            if name in kinds:
                @pl.when((idx >= base) & (idx < base + n_d))
                def _():
                    t = idx - base
                    down_copy(t % local_n, t // local_n, idx).start()
        if 'w' in kinds:
            @pl.when((idx >= at_w) & (idx < at_end))
            def _():
                tall_copy(wqkv_ref.at[:, cols(idx - at_w)], idx).start()

    def tall(idx):
        tall_copy(wo_ref.at[:, pl.ds(0, WIDE)], idx).wait()
        return ring[lax.rem(idx, RING)]

    lo, hi = pl.ds(0, half), pl.ds(half, half)

    def ag(m, k):
        own = xbuf.at[0, 0] if m == 0 else ubuf
        src, dst, to = (
            (own.at[lo], xbuf.at[1, 0, lo], right),
            (own.at[hi], xbuf.at[1, 0, hi], right),
            (own.at[hi], xbuf.at[2, 0, hi], left),
            (own.at[lo], xbuf.at[2, 0, lo], left),
            (own, xbuf.at[0, 1], partner),
            (xbuf.at[1, 0, lo], xbuf.at[3, 0, lo], right),
            (xbuf.at[2, 0, hi], xbuf.at[3, 0, hi], left),
            (xbuf.at[1, 0], xbuf.at[1, 1], partner),
            (xbuf.at[2, 0], xbuf.at[2, 1], partner),
            (xbuf.at[3, 0, lo], xbuf.at[3, 1, lo], partner),
            (xbuf.at[3, 0, hi], xbuf.at[3, 1, hi], partner),
        )[k]
        return pltpu.make_async_remote_copy(src_ref=src, dst_ref=dst, send_sem=ag_send.at[m, k], recv_sem=ag_recv.at[m, k],
                                            device_id={'ep': to}, device_id_type=pl.DeviceIdType.MESH)

    def meta(k):
        src, dst, to = (
            (mbuf.at[0, 0], mbuf.at[1, 0], right),
            (mbuf.at[0, 0], mbuf.at[2, 0], left),
            (mbuf.at[0, 0], mbuf.at[0, 1], partner),
            (mbuf.at[1, 0], mbuf.at[3, 0], right),
            (mbuf.at[1, 0], mbuf.at[1, 1], partner),
            (mbuf.at[2, 0], mbuf.at[2, 1], partner),
            (mbuf.at[3, 0], mbuf.at[3, 1], partner),
        )[k]
        return pltpu.make_async_remote_copy(src_ref=src, dst_ref=dst, send_sem=me_send.at[k], recv_sem=me_recv.at[k],
                                            device_id={'ep': to}, device_id_type=pl.DeviceIdType.MESH)

    def rs(k, q):
        src, dst, to = (
            (p1.at[lax.rem(q, 2)], dr.at[q], partner),
            (p0.at[q, 3, lo], ri.at[q, 0], right),
            (p0.at[q, 3, hi], ri.at[q, 1], left),
            (p0.at[q, 2, hi], fl.at[q, hi], right),
            (p0.at[q, 1, lo], fr.at[q, lo], left),
            (p0.at[q, 2, lo], fl.at[q, lo], right),
            (p0.at[q, 1, hi], fr.at[q, hi], left),
        )[k]
        return pltpu.make_async_remote_copy(src_ref=src, dst_ref=dst, send_sem=rs_send.at[q, k], recv_sem=rs_recv.at[q, k],
                                            device_id={'ep': to}, device_id_type=pl.DeviceIdType.MESH)

    def ag_own(m):
        for k in range(5):
            ag(m, k).start()

    def ag_relay(m):
        ag(m, 0).wait_recv()
        ag(m, 5).start()
        ag(m, 2).wait_recv()
        ag(m, 6).start()

    def ag_share(m):
        ag(m, 1).wait_recv()
        ag(m, 7).start()
        ag(m, 3).wait_recv()
        ag(m, 8).start()

    def ag_share_far(m):
        ag(m, 5).wait_recv()
        ag(m, 9).start()
        ag(m, 6).wait_recv()
        ag(m, 10).start()

    lane = lax.broadcasted_iota(jnp.int32, (local_n, n_slot), 1)
    owner = lax.broadcasted_iota(jnp.int32, (local_n, n_slot), 0)
    spread = jnp.where((lane >= owner * cap) & (lane < (owner + 1) * cap), 1.0, 0.0).astype(F32)

    def member_gate(m, o, j):
        ids = lax.broadcasted_iota(jnp.int32, (local_n, tok_n), 0).astype(F32) + first
        member = jnp.zeros((local_n, tok_n), F32)
        gate = jnp.zeros((local_n, tok_n), F32)
        for t in range(top_k):
            hit = mbuf[o, j, 16 * m + t:16 * m + t + 1, :] == ids
            member = jnp.where(hit, 1.0, member)
            gate = jnp.where(hit, mbuf[o, j, 16 * m + 8 + t:16 * m + 9 + t, :], gate)
        return member, gate

    def locate(m, o):
        tri = jnp.where(lax.broadcasted_iota(jnp.int32, (tok_n, tok_n), 0) < lax.broadcasted_iota(jnp.int32, (tok_n, tok_n), 1),
                        1.0, 0.0).astype(BF16)
        for j in range(2):
            member, _ = member_gate(m, o, j)
            rank = jnp.dot(member.astype(BF16), tri, preferred_element_type=F32)
            slots[o, :, j * tok_n:(j + 1) * tok_n] = jnp.where(member > 0.5, rank + float(j * cap), -1.0)

    def take(o, e0, e1):
        index = lax.broadcasted_iota(jnp.int32, (cap2, 2 * tok_n), 0).astype(F32)
        sel = jnp.concatenate([jnp.where(index == slots[o, e:e + 1, :], 1.0, 0.0) for e in range(e0, e1)], axis=0).astype(BF16)
        wide = 2 * WIDE
        both = xbuf[o].reshape(2 * tok_n, dim)
        for k in range(0, dim, wide):
            n = min(wide, dim - k)
            got = jnp.dot(sel, both[:, k:k + n], preferred_element_type=F32).astype(BF16)
            for e in range(e1 - e0):
                rows[e, o * cap2:(o + 1) * cap2, k:k + n] = got[e * cap2:(e + 1) * cap2, :]

    def weigh(m, o):
        pos = lax.rem(lax.broadcasted_iota(jnp.int32, (tok_n, n_slot), 1), cap).astype(F32)

        def over(a):
            return lax.dot_general(a, spread, (((0,), (0,)), ((), ())), preferred_element_type=F32)

        for j in range(2):
            member, rest = member_gate(m, o, j)
            slot = slots[o, :, j * tok_n:(j + 1) * tok_n]
            here = over(jnp.where(member > 0.5, slot - float(j * cap), -1.0)) == pos
            for part in range(3):
                head = rest.astype(BF16).astype(F32)
                gts[o, j, part] = jnp.where(here, over(head), 0.0).astype(BF16)
                rest = rest - head

    def gate_up(base, begin, end, kinds, events, both=False):
        def act(mine, at):
            gate = jnp.dot(mine, ring[lax.rem(at, RING)], preferred_element_type=F32)
            up = jnp.dot(mine, ring[lax.rem(at + 1, RING)], preferred_element_type=F32)
            return (jax.nn.silu(gate) * up).astype(BF16)

        def step(i, carry):
            at = base + 2 * i
            e, f = i // n_f, i % n_f
            tall_copy(wo_ref.at[:, pl.ds(0, WIDE)], at).wait()
            tall_copy(wo_ref.at[:, pl.ds(0, WIDE)], at + 1).wait()
            hidden[e, :, cols(f)] = act(rows[e], at)
            if both:
                k = e - (local_n - SHARED)
                later[k, :, cols(f)] = act(rows[k], at)
            fetch(at + RING, kinds)
            fetch(at + 1 + RING, kinds)
            events(i)
            return carry

        lax.fori_loop(begin, end, step, 0)

    def stage1(q):
        rs(0, q).wait_recv()
        for o in (3, 2, 1, 0):
            p0[q, o] = p0[q, o] + dr[q, o]
        for k in (1, 2, 3, 4):
            rs(k, q).start()

    def stage2(q):
        rs(1, q).wait_recv()
        rs(2, q).wait_recv()
        p0[q, 2, lo] = p0[q, 2, lo] + ri[q, 0]
        p0[q, 1, hi] = p0[q, 1, hi] + ri[q, 1]
        rs(5, q).start()
        rs(6, q).start()

    def combine(q):
        for o in range(n_pair):
            for j in (1, 0):
                total = None
                for part in range(3):
                    term = jnp.dot(gts[o, j, part], ys[o, j], preferred_element_type=F32)
                    total = term if total is None else total + term
                if j == 1:
                    p1[lax.rem(q, 2), o] = total
                else:
                    p0[q, o] = total

    def down(m, base, kinds):
        n_e = local_n // 2

        def step(i, carry):
            at = base + 2 * i
            q, e = i // n_e, i % n_e
            down_copy(0, 0, at).wait()
            down_copy(0, 0, at + 1).wait()
            y0 = jnp.dot(hidden[2 * e], ring[lax.rem(at, RING), pl.ds(0, ff)], preferred_element_type=F32)
            y1 = jnp.dot(hidden[2 * e + 1], ring[lax.rem(at + 1, RING), pl.ds(0, ff)], preferred_element_type=F32)
            for o in range(n_pair):
                for j in range(2):
                    here = slice(o * cap2 + j * cap, o * cap2 + (j + 1) * cap)
                    two = jnp.concatenate([y0[here], y1[here]], axis=0)
                    ys[o, j, pl.ds(pl.multiple_of(e * cap2, 16), cap2), :] = two.astype(BF16)
            fetch(at + RING, kinds)
            fetch(at + 1 + RING, kinds)

            if m == 1:
                @pl.when(e == 0)
                def _():
                    finish(0, q)
                    for peer in peers:
                        pl.semaphore_signal(rs_free.at[q], inc=1, device_id={'ep': peer}, device_id_type=pl.DeviceIdType.MESH)

            @pl.when((e == 1) & (q >= 1))
            def _():
                stage1(q - 1)

            @pl.when(e == n_e - 1)
            def _():
                @pl.when(q >= 2)
                def _():
                    rs(0, q - 2).wait_send()
                combine(q)
                if m == 1:
                    pl.semaphore_wait(rs_free.at[q], len(peers))
                rs(0, q).start()
            return carry

        lax.fori_loop(0, n_d // 2, step, 0)

    def finish(m, q):
        for k in (3, 4, 5, 6):
            rs(k, q).wait_recv()
        total = p0[q, 0] + fl[q] + fr[q]
        tokens, out = (abuf, abuf) if m == 0 else (ubuf, bbuf)
        out[:, cols(q)] = (tokens[:, cols(q)].astype(F32) + total).astype(BF16)
        for k in (1, 2, 3, 4, 5, 6):
            rs(k, q).wait_send()

    def io(k):
        src, dst = (
            (x_ref, xbuf.at[0, 0]),
            (attn_ref, bbuf),
            (h_ref, hbuf),
            (x_ref, abuf),
            (abuf, outa_ref),
            (bbuf, outb_ref),
            (qbuf, qkv_ref),
        )[k]
        return pltpu.make_async_copy(src, dst, io_sem.at[k])

    for k in range(3):
        io(k).start()
    for idx in range(RING):
        fetch(idx, ('o', 'ga'))
    barrier = pltpu.get_barrier_semaphore()
    signal_peers(barrier)
    mbuf[0, 0] = jnp.zeros_like(mbuf[0, 0])
    for at, ref in ((0, ra_ref), (8, ga_ref), (16, rb_ref), (24, gb_ref)):
        mbuf[0, 0, at:at + top_k, :] = ref[...].astype(F32)
    io(0).wait()
    pl.semaphore_wait(barrier, len(peers))
    for k in (0, 1, 2):
        meta(k).start()
    ag_own(0)
    io(1).wait()
    io(2).wait()
    io(3).start()

    def project(i, carry):
        proj = jnp.dot(bbuf[...], tall(i), preferred_element_type=F32).astype(BF16)
        ubuf[:, cols(i)] = (hbuf[:, cols(i)].astype(F32) + proj.astype(F32)).astype(BF16)
        fetch(i + RING, ('ga',))
        return carry

    lax.fori_loop(0, n_o, project, 0)
    meta(0).wait_recv()
    meta(3).start()
    meta(4).start()
    meta(1).wait_recv()
    meta(5).start()
    meta(2).wait_recv()
    ag(0, 4).wait_recv()
    locate(0, 0)
    take(0, 0, local_n)
    ag_relay(0)
    meta(3).wait_recv()
    meta(6).start()
    for k in (4, 5, 6):
        meta(k).wait_recv()
    for o in range(1, n_pair):
        locate(0, o)
    ag_share(0)
    ag(0, 7).wait_recv()
    take(1, 0, local_n)
    ag(0, 8).wait_recv()
    take(2, 0, local_n)
    for k in range(9):
        ag(0, k).wait_send()
    signal_peers(x_free.at[0])
    ag_share_far(0)
    pl.semaphore_wait(x_free.at[0], len(peers))
    ag_own(1)
    xbuf[0, 0] = ubuf[...]
    ag(0, 9).wait_recv()
    ag(0, 10).wait_recv()
    take(3, 0, local_n)
    for k in (9, 10):
        ag(0, k).wait_send()
    for k in range(7):
        meta(k).wait_send()
    signal_peers(x_free.at[1])

    def relay_b():
        pl.semaphore_wait(x_free.at[1], len(peers))
        ag_relay(1)

    def during_a(i):
        for when, event in ((6, relay_b), (11, lambda: ag_share(1)), (16, lambda: ag_share_far(1))):
            @pl.when(i == when)
            def _():
                event()

        @pl.when((i >= 7) & (i < 7 + n_pair))
        def _():
            weigh(0, i - 7)

    alone = (local_n - SHARED) * n_f
    gate_up(at_ga, 0, alone, ('ga',), during_a)
    for k in (4, 7, 8, 9, 10):
        ag(1, k).wait_recv()
    for o in range(n_pair):
        locate(1, o)
        take(o, local_n - SHARED, local_n)
    gate_up(at_ga, alone, n_ga, ('ga', 'da'), lambda i: None, both=True)
    down(0, at_da, ('da', 'gb'))
    for o in range(n_pair):
        take(o, 0, local_n - SHARED)
        if o == 1:
            stage1(n_q - 1)
    for k in range(SHARED):
        hidden[local_n - SHARED + k] = later[k]
    for q in (n_q - 2, n_q - 1):
        rs(0, q).wait_send()

    def during_b(i):
        @pl.when((i % 2 == 1) & (i < 2 * n_q))
        def _():
            stage2(i // 2)

        @pl.when((i >= 2 * n_q) & (i < 2 * n_q + n_pair))
        def _():
            weigh(1, i - 2 * n_q)

    io(3).wait()
    gate_up(at_gb, 0, n_gb, ('gb', 'db'), during_b)
    down(1, at_db, ('db', 'w'))
    io(4).start()

    def qkv(i, carry):
        qbuf[:, cols(i)] = jnp.dot(hbuf[...], tall(at_w + i), preferred_element_type=F32).astype(BF16)

        @pl.when(i == 1)
        def _():
            stage1(n_q - 1)

        @pl.when((i >= 2) & (i - 2 < n_q - 1))
        def _():
            stage2(i - 2)
        return carry

    lax.fori_loop(0, n_w, qkv, 0)
    io(6).start()
    stage2(n_q - 1)

    def last(q, carry):
        finish(1, q)
        return carry

    lax.fori_loop(0, n_q, last, 0)
    io(5).start()
    for q in (n_q - 2, n_q - 1):
        rs(0, q).wait_send()
    for k in range(11):
        ag(1, k).wait_send()
    for k in (4, 5, 6):
        io(k).wait()


def write_kernel(a_ref, b_ref, c_ref, oa_ref, ob_ref, oc_ref, va, vb, vc, sem_in, sem_out):
    moves = ((a_ref, va, oa_ref), (b_ref, vb, ob_ref), (c_ref, vc, oc_ref))
    for k, (src, buf, _) in enumerate(moves):
        pltpu.make_async_copy(src, buf, sem_in.at[k]).start()
    for k, (src, buf, dst) in enumerate(moves):
        pltpu.make_async_copy(src, buf, sem_in.at[k]).wait()
        pltpu.make_async_copy(buf, dst, sem_out.at[k]).start()
    for k, (_, buf, dst) in enumerate(moves):
        pltpu.make_async_copy(buf, dst, sem_out.at[k]).wait()


def write_out(arrays):
    hbm = pl.BlockSpec(memory_space=pl.ANY)
    return pl.pallas_call(
        write_kernel,
        out_shape=tuple(jax.ShapeDtypeStruct(a.shape, a.dtype) for a in arrays),
        in_specs=[hbm] * 3,
        out_specs=(hbm,) * 3,
        scratch_shapes=[pltpu.VMEM(a.shape, a.dtype) for a in arrays] + [pltpu.SemaphoreType.DMA((3,)), pltpu.SemaphoreType.DMA((3,))],
    )(*arrays)


def solution(mesh):
    n_devs = mesh.shape['ep']

    def local_step(x_a, route_a, gate_a, h_b, attn_b, route_b, gate_b, w_qkv, w_o, w_gate, w_up, w_down):
        tok_n, dim = x_a.shape
        top_k = route_a.shape[1]
        local_n, _, ff = w_gate.shape
        qkv_n = w_qkv.shape[1]
        n_experts = local_n * n_devs
        cap = min(tok_n, 2 * ((tok_n * top_k + n_experts - 1) // n_experts))
        n_pair = n_devs // 2
        n_q = dim // WIDE
        cap2 = 2 * cap
        m = n_pair * cap2
        half = tok_n // 2

        vmem = pl.BlockSpec(memory_space=pltpu.VMEM)
        hbm = pl.BlockSpec(memory_space=pl.ANY)
        flops = 2 * 2 * 3 * local_n * m * dim * ff
        weight_bytes = 2 * 6 * local_n * dim * ff
        results = pl.pallas_call(
            functools.partial(moe_kernel, n_devs, top_k, cap),
            out_shape=(
                jax.ShapeDtypeStruct((tok_n, dim), BF16),
                jax.ShapeDtypeStruct((tok_n, dim), BF16),
                jax.ShapeDtypeStruct((tok_n, qkv_n), BF16),
            ),
            in_specs=[vmem] * 4 + [hbm] * 8,
            out_specs=(hbm, hbm, hbm),
            scratch_shapes=[
                pltpu.VMEM((RING, dim, WIDE), BF16),
                pltpu.VMEM((n_pair, 2, tok_n, dim), BF16),
                pltpu.VMEM((n_pair, 2, 32, tok_n), F32),
                pltpu.VMEM((tok_n, dim), BF16),
                pltpu.VMEM((tok_n, dim), BF16),
                pltpu.VMEM((tok_n, dim), BF16),
                pltpu.VMEM((tok_n, dim), BF16),
                pltpu.VMEM((tok_n, qkv_n), BF16),
                pltpu.VMEM((local_n, m, dim), BF16),
                pltpu.VMEM((local_n, m, ff), BF16),
                pltpu.VMEM((SHARED, m, ff), BF16),
                pltpu.VMEM((n_pair, local_n, 2 * tok_n), F32),
                pltpu.VMEM((n_pair, 2, 3, tok_n, local_n * cap), BF16),
                pltpu.VMEM((n_pair, 2, local_n * cap, WIDE), BF16),
                pltpu.VMEM((n_q, n_pair, tok_n, WIDE), F32),
                pltpu.VMEM((2, n_pair, tok_n, WIDE), F32),
                pltpu.VMEM((n_q, n_pair, tok_n, WIDE), F32),
                pltpu.VMEM((n_q, 2, half, WIDE), F32),
                pltpu.VMEM((n_q, tok_n, WIDE), F32),
                pltpu.VMEM((n_q, tok_n, WIDE), F32),
                pltpu.SemaphoreType.DMA((RING,)),
                pltpu.SemaphoreType.DMA((7,)),
                pltpu.SemaphoreType.DMA((2, 11)),
                pltpu.SemaphoreType.DMA((2, 11)),
                pltpu.SemaphoreType.DMA((7,)),
                pltpu.SemaphoreType.DMA((7,)),
                pltpu.SemaphoreType.DMA((n_q, 7)),
                pltpu.SemaphoreType.DMA((n_q, 7)),
                pltpu.SemaphoreType.REGULAR((2,)),
                pltpu.SemaphoreType.REGULAR((n_q,)),
            ],
            compiler_params=pltpu.CompilerParams(collective_id=0, has_side_effects=True, vmem_limit_bytes=67043328),
            cost_estimate=pl.CostEstimate(flops=flops, bytes_accessed=weight_bytes, transcendentals=0),
        )(route_a.T, gate_a.T, route_b.T, gate_b.T, x_a, h_b, attn_b, w_qkv, w_o, w_gate, w_up, w_down)
        return write_out(results)

    row_spec = P(('dp', 'ep'), None)
    full_spec = P(None, None)
    expert_spec = P('ep', None, None)
    return jax.shard_map(
        local_step,
        mesh=mesh,
        in_specs=(row_spec, row_spec, row_spec, row_spec, row_spec, row_spec, row_spec, full_spec, full_spec, expert_spec, expert_spec, expert_spec),
        out_specs=(row_spec, row_spec, row_spec),
        check_vma=False,
    )
```

```python
import functools

import jax
import jax.numpy as jnp
from jax import lax
from jax.experimental import pallas as pl
from jax.experimental.pallas import tpu as pltpu
from jax.sharding import PartitionSpec as P

F32 = jnp.float32
BF16 = jnp.bfloat16
RING = 8
WIDE = 512
SHARED = 2


def moe_kernel(n_devs, top_k, cap, ra_ref, ga_ref, rb_ref, gb_ref, x_ref, h_ref, attn_ref,
               wqkv_ref, wo_ref, wg_ref, wu_ref, wd_ref,
               outa_ref, outb_ref, qkv_ref,
               ring, xbuf, near, mbuf, ubuf, abuf, bbuf, hbuf, qbuf, rows, hidden, later, slots, gts, ys, p0, p1, dr, ri, fl, fr,
               ring_sem, io_sem, ag_send, ag_recv, me_send, me_recv, rs_send, rs_recv, x_free, rs_free):
    tok_n, dim = x_ref.shape
    half = tok_n // 2
    local_n, _, ff = wg_ref.shape
    qkv_n = wqkv_ref.shape[1]
    cap2 = 2 * cap
    n_pair = n_devs // 2
    n_slot = local_n * cap
    me = lax.axis_index('ep')
    core = lax.rem(me, 2)
    partner = me + 1 - 2 * core
    right = lax.rem(me + 2, n_devs)
    left = lax.rem(me + n_devs - 2, n_devs)
    first = (me * local_n).astype(F32)
    peers = (partner, left, right)

    def signal_peers(sem):
        for peer in peers:
            pl.semaphore_signal(sem, inc=1, device_id={'ep': peer}, device_id_type=pl.DeviceIdType.MESH)

    n_o, n_f, n_q, n_w = dim // WIDE, ff // WIDE, dim // WIDE, qkv_n // WIDE
    n_ga, n_gb, n_d = local_n * n_f, (local_n - SHARED) * n_f, local_n * n_q
    at_ga = n_o
    at_da = at_ga + 2 * n_ga
    at_gb = at_da + n_d
    at_db = at_gb + 2 * n_gb
    at_w = at_db + n_d
    at_end = at_w + n_w

    def cols(k):
        return pl.ds(pl.multiple_of(k * WIDE, WIDE), WIDE)

    def tall_copy(src, idx):
        slot = lax.rem(idx, RING)
        return pltpu.make_async_copy(src, ring.at[slot], ring_sem.at[slot])

    def down_copy(e, k, idx):
        slot = lax.rem(idx, RING)
        return pltpu.make_async_copy(wd_ref.at[e, :, cols(k)], ring.at[slot, pl.ds(0, ff)], ring_sem.at[slot])

    def start_gu(t, idx):
        step = t // 2
        e, f = step // n_f, step % n_f

        @pl.when(t % 2 == 0)
        def _():
            tall_copy(wg_ref.at[e, :, cols(f)], idx).start()

        @pl.when(t % 2 == 1)
        def _():
            tall_copy(wu_ref.at[e, :, cols(f)], idx).start()

    def fetch(idx, kinds):
        if 'o' in kinds:
            @pl.when(idx < at_ga)
            def _():
                tall_copy(wo_ref.at[:, cols(idx)], idx).start()
        for name, base, steps in (('ga', at_ga, n_ga), ('gb', at_gb, n_gb)):
            if name in kinds:
                @pl.when((idx >= base) & (idx < base + 2 * steps))
                def _():
                    start_gu(idx - base, idx)
        for name, base in (('da', at_da), ('db', at_db)):
            if name in kinds:
                @pl.when((idx >= base) & (idx < base + n_d))
                def _():
                    t = idx - base
                    down_copy(t % local_n, t // local_n, idx).start()
        if 'w' in kinds:
            @pl.when((idx >= at_w) & (idx < at_end))
            def _():
                tall_copy(wqkv_ref.at[:, cols(idx - at_w)], idx).start()

    def tall(idx):
        tall_copy(wo_ref.at[:, pl.ds(0, WIDE)], idx).wait()
        return ring[lax.rem(idx, RING)]

    lo, hi = pl.ds(0, half), pl.ds(half, half)

    def ag(m, k):
        own, from_left, from_right = (xbuf.at[0, 0], xbuf.at[1, 0], xbuf.at[2, 0]) if m == 0 else (ubuf, near.at[0], near.at[1])
        src, dst, to = (
            (own.at[lo], from_left.at[lo], right),
            (own.at[hi], from_left.at[hi], right),
            (own.at[hi], from_right.at[hi], left),
            (own.at[lo], from_right.at[lo], left),
            (own, xbuf.at[0, 1], partner),
            (from_left.at[lo], xbuf.at[3, 0, lo], right),
            (from_right.at[hi], xbuf.at[3, 0, hi], left),
            (from_left, xbuf.at[1, 1], partner),
            (from_right, xbuf.at[2, 1], partner),
            (xbuf.at[3, 0, lo], xbuf.at[3, 1, lo], partner),
            (xbuf.at[3, 0, hi], xbuf.at[3, 1, hi], partner),
        )[k]
        return pltpu.make_async_remote_copy(src_ref=src, dst_ref=dst, send_sem=ag_send.at[m, k], recv_sem=ag_recv.at[m, k],
                                            device_id={'ep': to}, device_id_type=pl.DeviceIdType.MESH)

    def meta(k):
        src, dst, to = (
            (mbuf.at[0, 0], mbuf.at[1, 0], right),
            (mbuf.at[0, 0], mbuf.at[2, 0], left),
            (mbuf.at[0, 0], mbuf.at[0, 1], partner),
            (mbuf.at[1, 0], mbuf.at[3, 0], right),
            (mbuf.at[1, 0], mbuf.at[1, 1], partner),
            (mbuf.at[2, 0], mbuf.at[2, 1], partner),
            (mbuf.at[3, 0], mbuf.at[3, 1], partner),
        )[k]
        return pltpu.make_async_remote_copy(src_ref=src, dst_ref=dst, send_sem=me_send.at[k], recv_sem=me_recv.at[k],
                                            device_id={'ep': to}, device_id_type=pl.DeviceIdType.MESH)

    def rs(k, q):
        src, dst, to = (
            (p1.at[lax.rem(q, 2)], dr.at[q], partner),
            (p0.at[q, 3, lo], ri.at[q, 0], right),
            (p0.at[q, 3, hi], ri.at[q, 1], left),
            (p0.at[q, 2, hi], fl.at[q, hi], right),
            (p0.at[q, 1, lo], fr.at[q, lo], left),
            (p0.at[q, 2, lo], fl.at[q, lo], right),
            (p0.at[q, 1, hi], fr.at[q, hi], left),
        )[k]
        return pltpu.make_async_remote_copy(src_ref=src, dst_ref=dst, send_sem=rs_send.at[q, k], recv_sem=rs_recv.at[q, k],
                                            device_id={'ep': to}, device_id_type=pl.DeviceIdType.MESH)

    def ag_own(m):
        for k in range(4):
            ag(m, k).start()

    def ag_relay(m):
        ag(m, 0).wait_recv()
        ag(m, 5).start()
        ag(m, 2).wait_recv()
        ag(m, 6).start()

    def ag_share(m):
        ag(m, 1).wait_recv()
        ag(m, 7).start()
        ag(m, 3).wait_recv()
        ag(m, 8).start()

    def ag_share_far(m):
        ag(m, 5).wait_recv()
        ag(m, 9).start()
        ag(m, 6).wait_recv()
        ag(m, 10).start()

    lane = lax.broadcasted_iota(jnp.int32, (local_n, n_slot), 1)
    owner = lax.broadcasted_iota(jnp.int32, (local_n, n_slot), 0)
    spread = jnp.where((lane >= owner * cap) & (lane < (owner + 1) * cap), 1.0, 0.0).astype(F32)

    def member_gate(m, o, j):
        ids = lax.broadcasted_iota(jnp.int32, (local_n, tok_n), 0).astype(F32) + first
        member = jnp.zeros((local_n, tok_n), F32)
        gate = jnp.zeros((local_n, tok_n), F32)
        for t in range(top_k):
            hit = mbuf[o, j, 16 * m + t:16 * m + t + 1, :] == ids
            member = jnp.where(hit, 1.0, member)
            gate = jnp.where(hit, mbuf[o, j, 16 * m + 8 + t:16 * m + 9 + t, :], gate)
        return member, gate

    def locate(m, o):
        tri = jnp.where(lax.broadcasted_iota(jnp.int32, (tok_n, tok_n), 0) < lax.broadcasted_iota(jnp.int32, (tok_n, tok_n), 1),
                        1.0, 0.0).astype(BF16)
        for j in range(2):
            member, _ = member_gate(m, o, j)
            rank = jnp.dot(member.astype(BF16), tri, preferred_element_type=F32)
            slots[o, :, j * tok_n:(j + 1) * tok_n] = jnp.where(member > 0.5, rank + float(j * cap), -1.0)

    def take(o, e0, e1):
        index = lax.broadcasted_iota(jnp.int32, (cap2, 2 * tok_n), 0).astype(F32)
        sel = jnp.concatenate([jnp.where(index == slots[o, e:e + 1, :], 1.0, 0.0) for e in range(e0, e1)], axis=0).astype(BF16)
        wide = 2 * WIDE
        both = xbuf[o].reshape(2 * tok_n, dim)
        for k in range(0, dim, wide):
            n = min(wide, dim - k)
            got = jnp.dot(sel, both[:, k:k + n], preferred_element_type=F32).astype(BF16)
            for e in range(e1 - e0):
                rows[e, o * cap2:(o + 1) * cap2, k:k + n] = got[e * cap2:(e + 1) * cap2, :]

    def weigh(m, o):
        pos = lax.rem(lax.broadcasted_iota(jnp.int32, (tok_n, n_slot), 1), cap).astype(F32)

        def over(a):
            return lax.dot_general(a, spread, (((0,), (0,)), ((), ())), preferred_element_type=F32)

        for j in range(2):
            member, rest = member_gate(m, o, j)
            slot = slots[o, :, j * tok_n:(j + 1) * tok_n]
            here = over(jnp.where(member > 0.5, slot - float(j * cap), -1.0)) == pos
            for part in range(3):
                head = rest.astype(BF16).astype(F32)
                gts[o, j, part] = jnp.where(here, over(head), 0.0).astype(BF16)
                rest = rest - head

    def gate_up(base, begin, end, kinds, events, both=False):
        def act(mine, at):
            gate = jnp.dot(mine, ring[lax.rem(at, RING)], preferred_element_type=F32)
            up = jnp.dot(mine, ring[lax.rem(at + 1, RING)], preferred_element_type=F32)
            return (jax.nn.silu(gate) * up).astype(BF16)

        def step(i, carry):
            at = base + 2 * i
            e, f = i // n_f, i % n_f
            tall_copy(wo_ref.at[:, pl.ds(0, WIDE)], at).wait()
            tall_copy(wo_ref.at[:, pl.ds(0, WIDE)], at + 1).wait()
            hidden[e, :, cols(f)] = act(rows[e], at)
            if both:
                k = e - (local_n - SHARED)
                later[k, :, cols(f)] = act(rows[k], at)
            fetch(at + RING, kinds)
            fetch(at + 1 + RING, kinds)
            events(i)
            return carry

        lax.fori_loop(begin, end, step, 0)

    def stage1(q):
        rs(0, q).wait_recv()
        for o in (3, 2, 1, 0):
            p0[q, o] = p0[q, o] + dr[q, o]
        for k in (1, 2, 3, 4):
            rs(k, q).start()

    def stage2(q):
        rs(1, q).wait_recv()
        rs(2, q).wait_recv()
        p0[q, 2, lo] = p0[q, 2, lo] + ri[q, 0]
        p0[q, 1, hi] = p0[q, 1, hi] + ri[q, 1]
        rs(5, q).start()
        rs(6, q).start()

    def combine(q):
        for o in range(n_pair):
            for j in (1, 0):
                total = None
                for part in range(3):
                    term = jnp.dot(gts[o, j, part], ys[o, j], preferred_element_type=F32)
                    total = term if total is None else total + term
                if j == 1:
                    p1[lax.rem(q, 2), o] = total
                else:
                    p0[q, o] = total

    def down(m, base, kinds):
        n_e = local_n // 2

        def step(i, carry):
            at = base + 2 * i
            q, e = i // n_e, i % n_e
            down_copy(0, 0, at).wait()
            down_copy(0, 0, at + 1).wait()
            y0 = jnp.dot(hidden[2 * e], ring[lax.rem(at, RING), pl.ds(0, ff)], preferred_element_type=F32)
            y1 = jnp.dot(hidden[2 * e + 1], ring[lax.rem(at + 1, RING), pl.ds(0, ff)], preferred_element_type=F32)
            for o in range(n_pair):
                for j in range(2):
                    here = slice(o * cap2 + j * cap, o * cap2 + (j + 1) * cap)
                    two = jnp.concatenate([y0[here], y1[here]], axis=0)
                    ys[o, j, pl.ds(pl.multiple_of(e * cap2, 16), cap2), :] = two.astype(BF16)
            fetch(at + RING, kinds)
            fetch(at + 1 + RING, kinds)

            if m == 1:
                @pl.when(e == 0)
                def _():
                    finish(0, q)
                    for peer in peers:
                        pl.semaphore_signal(rs_free.at[q], inc=1, device_id={'ep': peer}, device_id_type=pl.DeviceIdType.MESH)

            @pl.when((e == 1) & (q >= 1))
            def _():
                stage1(q - 1)

            @pl.when(e == n_e - 1)
            def _():
                @pl.when(q >= 2)
                def _():
                    rs(0, q - 2).wait_send()
                combine(q)
                if m == 1:
                    pl.semaphore_wait(rs_free.at[q], len(peers))
                rs(0, q).start()
            return carry

        lax.fori_loop(0, n_d // 2, step, 0)

    def finish(m, q):
        for k in (3, 4, 5, 6):
            rs(k, q).wait_recv()
        total = p0[q, 0] + fl[q] + fr[q]
        tokens, out = (abuf, abuf) if m == 0 else (ubuf, bbuf)
        out[:, cols(q)] = (tokens[:, cols(q)].astype(F32) + total).astype(BF16)
        for k in (1, 2, 3, 4, 5, 6):
            rs(k, q).wait_send()

    def io(k):
        src, dst = (
            (x_ref, xbuf.at[0, 0]),
            (attn_ref, bbuf),
            (h_ref, hbuf),
            (x_ref, abuf),
            (abuf, outa_ref),
            (bbuf, outb_ref),
            (qbuf, qkv_ref),
        )[k]
        return pltpu.make_async_copy(src, dst, io_sem.at[k])

    for k in range(3):
        io(k).start()
    for idx in range(RING):
        fetch(idx, ('o', 'ga'))
    barrier = pltpu.get_barrier_semaphore()
    signal_peers(barrier)
    mbuf[0, 0] = jnp.zeros_like(mbuf[0, 0])
    for at, ref in ((0, ra_ref), (8, ga_ref), (16, rb_ref), (24, gb_ref)):
        mbuf[0, 0, at:at + top_k, :] = ref[...].astype(F32)
    io(0).wait()
    pl.semaphore_wait(barrier, len(peers))
    for k in (0, 1, 2):
        meta(k).start()
    ag_own(0)
    ag(0, 4).start()
    io(1).wait()
    io(2).wait()
    io(3).start()

    def project(i, carry):
        proj = jnp.dot(bbuf[...], tall(i), preferred_element_type=F32).astype(BF16)
        ubuf[:, cols(i)] = (hbuf[:, cols(i)].astype(F32) + proj.astype(F32)).astype(BF16)
        fetch(i + RING, ('ga',))
        return carry

    lax.fori_loop(0, n_o, project, 0)
    meta(0).wait_recv()
    meta(3).start()
    meta(4).start()
    meta(1).wait_recv()
    meta(5).start()
    meta(2).wait_recv()
    ag(0, 4).wait_recv()
    locate(0, 0)
    take(0, 0, local_n)
    ag_relay(0)
    ag_own(1)
    meta(3).wait_recv()
    meta(6).start()
    for k in (4, 5, 6):
        meta(k).wait_recv()
    for o in range(1, n_pair):
        locate(0, o)
    ag_share(0)
    ag(0, 7).wait_recv()
    take(1, 0, local_n)
    ag(0, 8).wait_recv()
    take(2, 0, local_n)
    ag_share_far(0)
    ag(0, 9).wait_recv()
    ag(0, 10).wait_recv()
    take(3, 0, local_n)
    for k in range(11):
        ag(0, k).wait_send()
    for k in range(7):
        meta(k).wait_send()
    signal_peers(x_free)
    xbuf[0, 0] = ubuf[...]

    def relay_b():
        pl.semaphore_wait(x_free, len(peers))
        ag(1, 4).start()
        ag_relay(1)

    def during_a(i):
        for when, event in ((6, relay_b), (11, lambda: ag_share(1)), (16, lambda: ag_share_far(1))):
            @pl.when(i == when)
            def _():
                event()

        @pl.when((i >= 7) & (i < 7 + n_pair))
        def _():
            weigh(0, i - 7)

    alone = (local_n - SHARED) * n_f
    gate_up(at_ga, 0, alone, ('ga',), during_a)
    for k in (4, 7, 8, 9, 10):
        ag(1, k).wait_recv()
    for o in range(n_pair):
        if o in (1, 2):
            xbuf[o, 0] = near[o - 1]
        locate(1, o)
        take(o, local_n - SHARED, local_n)
    gate_up(at_ga, alone, n_ga, ('ga', 'da'), lambda i: None, both=True)
    down(0, at_da, ('da', 'gb'))
    for o in range(n_pair):
        take(o, 0, local_n - SHARED)
        if o == 1:
            stage1(n_q - 1)
    for k in range(SHARED):
        hidden[local_n - SHARED + k] = later[k]
    for q in (n_q - 2, n_q - 1):
        rs(0, q).wait_send()

    def during_b(i):
        @pl.when((i % 3 == 2) & (i < 3 * n_q))
        def _():
            stage2(i // 3)

        @pl.when((i >= 12) & (i < 12 + n_pair))
        def _():
            weigh(1, i - 12)

    io(3).wait()
    gate_up(at_gb, 0, n_gb, ('gb', 'db'), during_b)
    down(1, at_db, ('db', 'w'))
    io(4).start()

    def qkv(i, carry):
        qbuf[:, cols(i)] = jnp.dot(hbuf[...], tall(at_w + i), preferred_element_type=F32).astype(BF16)

        @pl.when(i == 1)
        def _():
            stage1(n_q - 1)

        @pl.when((i >= 2) & (i - 2 < n_q - 1))
        def _():
            stage2(i - 2)
        return carry

    lax.fori_loop(0, n_w, qkv, 0)
    io(6).start()
    stage2(n_q - 1)

    def last(q, carry):
        finish(1, q)
        return carry

    lax.fori_loop(0, n_q, last, 0)
    io(5).start()
    for q in (n_q - 2, n_q - 1):
        rs(0, q).wait_send()
    for k in range(11):
        ag(1, k).wait_send()
    for k in (4, 5, 6):
        io(k).wait()


def write_kernel(a_ref, b_ref, c_ref, oa_ref, ob_ref, oc_ref, va, vb, vc, sem_in, sem_out):
    moves = ((a_ref, va, oa_ref), (b_ref, vb, ob_ref), (c_ref, vc, oc_ref))
    for k, (src, buf, _) in enumerate(moves):
        pltpu.make_async_copy(src, buf, sem_in.at[k]).start()
    for k, (src, buf, dst) in enumerate(moves):
        pltpu.make_async_copy(src, buf, sem_in.at[k]).wait()
        pltpu.make_async_copy(buf, dst, sem_out.at[k]).start()
    for k, (_, buf, dst) in enumerate(moves):
        pltpu.make_async_copy(buf, dst, sem_out.at[k]).wait()


def write_out(arrays):
    hbm = pl.BlockSpec(memory_space=pl.ANY)
    return pl.pallas_call(
        write_kernel,
        out_shape=tuple(jax.ShapeDtypeStruct(a.shape, a.dtype) for a in arrays),
        in_specs=[hbm] * 3,
        out_specs=(hbm,) * 3,
        scratch_shapes=[pltpu.VMEM(a.shape, a.dtype) for a in arrays] + [pltpu.SemaphoreType.DMA((3,)), pltpu.SemaphoreType.DMA((3,))],
    )(*arrays)


def solution(mesh):
    n_devs = mesh.shape['ep']

    def local_step(x_a, route_a, gate_a, h_b, attn_b, route_b, gate_b, w_qkv, w_o, w_gate, w_up, w_down):
        tok_n, dim = x_a.shape
        top_k = route_a.shape[1]
        local_n, _, ff = w_gate.shape
        qkv_n = w_qkv.shape[1]
        n_experts = local_n * n_devs
        cap = min(tok_n, 2 * ((tok_n * top_k + n_experts - 1) // n_experts))
        n_pair = n_devs // 2
        n_q = dim // WIDE
        cap2 = 2 * cap
        m = n_pair * cap2
        half = tok_n // 2

        vmem = pl.BlockSpec(memory_space=pltpu.VMEM)
        hbm = pl.BlockSpec(memory_space=pl.ANY)
        flops = 2 * 2 * 3 * local_n * m * dim * ff
        weight_bytes = 2 * 6 * local_n * dim * ff
        results = pl.pallas_call(
            functools.partial(moe_kernel, n_devs, top_k, cap),
            out_shape=(
                jax.ShapeDtypeStruct((tok_n, dim), BF16),
                jax.ShapeDtypeStruct((tok_n, dim), BF16),
                jax.ShapeDtypeStruct((tok_n, qkv_n), BF16),
            ),
            in_specs=[vmem] * 4 + [hbm] * 8,
            out_specs=(hbm, hbm, hbm),
            scratch_shapes=[
                pltpu.VMEM((RING, dim, WIDE), BF16),
                pltpu.VMEM((n_pair, 2, tok_n, dim), BF16),
                pltpu.VMEM((2, tok_n, dim), BF16),
                pltpu.VMEM((n_pair, 2, 32, tok_n), F32),
                pltpu.VMEM((tok_n, dim), BF16),
                pltpu.VMEM((tok_n, dim), BF16),
                pltpu.VMEM((tok_n, dim), BF16),
                pltpu.VMEM((tok_n, dim), BF16),
                pltpu.VMEM((tok_n, qkv_n), BF16),
                pltpu.VMEM((local_n, m, dim), BF16),
                pltpu.VMEM((local_n, m, ff), BF16),
                pltpu.VMEM((SHARED, m, ff), BF16),
                pltpu.VMEM((n_pair, local_n, 2 * tok_n), F32),
                pltpu.VMEM((n_pair, 2, 3, tok_n, local_n * cap), BF16),
                pltpu.VMEM((n_pair, 2, local_n * cap, WIDE), BF16),
                pltpu.VMEM((n_q, n_pair, tok_n, WIDE), F32),
                pltpu.VMEM((2, n_pair, tok_n, WIDE), F32),
                pltpu.VMEM((n_q, n_pair, tok_n, WIDE), F32),
                pltpu.VMEM((n_q, 2, half, WIDE), F32),
                pltpu.VMEM((n_q, tok_n, WIDE), F32),
                pltpu.VMEM((n_q, tok_n, WIDE), F32),
                pltpu.SemaphoreType.DMA((RING,)),
                pltpu.SemaphoreType.DMA((7,)),
                pltpu.SemaphoreType.DMA((2, 11)),
                pltpu.SemaphoreType.DMA((2, 11)),
                pltpu.SemaphoreType.DMA((7,)),
                pltpu.SemaphoreType.DMA((7,)),
                pltpu.SemaphoreType.DMA((n_q, 7)),
                pltpu.SemaphoreType.DMA((n_q, 7)),
                pltpu.SemaphoreType.REGULAR,
                pltpu.SemaphoreType.REGULAR((n_q,)),
            ],
            compiler_params=pltpu.CompilerParams(collective_id=0, has_side_effects=True, vmem_limit_bytes=67043328),
            cost_estimate=pl.CostEstimate(flops=flops, bytes_accessed=weight_bytes, transcendentals=0),
        )(route_a.T, gate_a.T, route_b.T, gate_b.T, x_a, h_b, attn_b, w_qkv, w_o, w_gate, w_up, w_down)
        return write_out(results)

    row_spec = P(('dp', 'ep'), None)
    full_spec = P(None, None)
    expert_spec = P('ep', None, None)
    return jax.shard_map(
        local_step,
        mesh=mesh,
        in_specs=(row_spec, row_spec, row_spec, row_spec, row_spec, row_spec, row_spec, full_spec, full_spec, expert_spec, expert_spec, expert_spec),
        out_specs=(row_spec, row_spec, row_spec),
        check_vma=False,
    )
```

```python
import functools

import jax
import jax.numpy as jnp
from jax import lax
from jax.experimental import pallas as pl
from jax.experimental.pallas import tpu as pltpu
from jax.sharding import PartitionSpec as P

F32 = jnp.float32
BF16 = jnp.bfloat16
RING = 8
WIDE = 512
SHARED = 1


def moe_kernel(n_devs, top_k, cap, ra_ref, ga_ref, rb_ref, gb_ref, x_ref, h_ref, attn_ref,
               wqkv_ref, wo_ref, wg_ref, wu_ref, wd_ref,
               outa_ref, outb_ref, qkv_ref,
               ring, xbuf, near, mbuf, ubuf, abuf, bbuf, hbuf, rows, hidden, later, slots, gts, ys, p0, p1, dr, ri, fl, fr,
               ring_sem, io_sem, ag_send, ag_recv, me_send, me_recv, rs_send, rs_recv, x_free, rs_free):
    tok_n, dim = x_ref.shape
    half = tok_n // 2
    local_n, _, ff = wg_ref.shape
    qkv_n = wqkv_ref.shape[1]
    cap2 = 2 * cap
    n_pair = n_devs // 2
    n_slot = local_n * cap
    me = lax.axis_index('ep')
    core = lax.rem(me, 2)
    partner = me + 1 - 2 * core
    right = lax.rem(me + 2, n_devs)
    left = lax.rem(me + n_devs - 2, n_devs)
    first = (me * local_n).astype(F32)
    peers = (partner, left, right)

    def signal_peers(sem):
        for peer in peers:
            pl.semaphore_signal(sem, inc=1, device_id={'ep': peer}, device_id_type=pl.DeviceIdType.MESH)

    n_o, n_f, n_q, n_w = dim // WIDE, ff // WIDE, dim // WIDE, qkv_n // WIDE
    n_ga, n_gb, n_d = local_n * n_f, (local_n - SHARED) * n_f, local_n * n_q
    at_ga = n_o
    at_da = at_ga + 2 * n_ga
    at_gb = at_da + n_d
    at_db = at_gb + 2 * n_gb
    at_w = at_db + n_d
    at_end = at_w + n_w

    def cols(k):
        return pl.ds(pl.multiple_of(k * WIDE, WIDE), WIDE)

    def tall_copy(src, idx):
        slot = lax.rem(idx, RING)
        return pltpu.make_async_copy(src, ring.at[slot], ring_sem.at[slot])

    def down_copy(e, k, idx):
        slot = lax.rem(idx, RING)
        return pltpu.make_async_copy(wd_ref.at[e, :, cols(k)], ring.at[slot, pl.ds(0, ff)], ring_sem.at[slot])

    def start_gu(t, idx):
        step = t // 2
        e, f = step // n_f, step % n_f

        @pl.when(t % 2 == 0)
        def _():
            tall_copy(wg_ref.at[e, :, cols(f)], idx).start()

        @pl.when(t % 2 == 1)
        def _():
            tall_copy(wu_ref.at[e, :, cols(f)], idx).start()

    def fetch(idx, kinds):
        if 'o' in kinds:
            @pl.when(idx < at_ga)
            def _():
                tall_copy(wo_ref.at[:, cols(idx)], idx).start()
        for name, base, steps in (('ga', at_ga, n_ga), ('gb', at_gb, n_gb)):
            if name in kinds:
                @pl.when((idx >= base) & (idx < base + 2 * steps))
                def _():
                    start_gu(idx - base, idx)
        for name, base in (('da', at_da), ('db', at_db)):
            if name in kinds:
                @pl.when((idx >= base) & (idx < base + n_d))
                def _():
                    t = idx - base
                    down_copy(t % local_n, t // local_n, idx).start()
        if 'w' in kinds:
            @pl.when((idx >= at_w) & (idx < at_end))
            def _():
                tall_copy(wqkv_ref.at[:, cols(idx - at_w)], idx).start()

    def tall(idx):
        tall_copy(wo_ref.at[:, pl.ds(0, WIDE)], idx).wait()
        return ring[lax.rem(idx, RING)]

    lo, hi = pl.ds(0, half), pl.ds(half, half)

    def ag(m, k):
        own, from_left, from_right = (xbuf.at[0, 0], xbuf.at[1, 0], xbuf.at[2, 0]) if m == 0 else (ubuf, near.at[0], near.at[1])
        src, dst, to = (
            (own.at[lo], from_left.at[lo], right),
            (own.at[hi], from_left.at[hi], right),
            (own.at[hi], from_right.at[hi], left),
            (own.at[lo], from_right.at[lo], left),
            (own, xbuf.at[0, 1], partner),
            (from_left.at[lo], xbuf.at[3, 0, lo], right),
            (from_right.at[hi], xbuf.at[3, 0, hi], left),
            (from_left, xbuf.at[1, 1], partner),
            (from_right, xbuf.at[2, 1], partner),
            (xbuf.at[3, 0, lo], xbuf.at[3, 1, lo], partner),
            (xbuf.at[3, 0, hi], xbuf.at[3, 1, hi], partner),
        )[k]
        return pltpu.make_async_remote_copy(src_ref=src, dst_ref=dst, send_sem=ag_send.at[m, k], recv_sem=ag_recv.at[m, k],
                                            device_id={'ep': to}, device_id_type=pl.DeviceIdType.MESH)

    def meta(k):
        src, dst, to = (
            (mbuf.at[0, 0], mbuf.at[1, 0], right),
            (mbuf.at[0, 0], mbuf.at[2, 0], left),
            (mbuf.at[0, 0], mbuf.at[0, 1], partner),
            (mbuf.at[1, 0], mbuf.at[3, 0], right),
            (mbuf.at[1, 0], mbuf.at[1, 1], partner),
            (mbuf.at[2, 0], mbuf.at[2, 1], partner),
            (mbuf.at[3, 0], mbuf.at[3, 1], partner),
        )[k]
        return pltpu.make_async_remote_copy(src_ref=src, dst_ref=dst, send_sem=me_send.at[k], recv_sem=me_recv.at[k],
                                            device_id={'ep': to}, device_id_type=pl.DeviceIdType.MESH)

    def rs(k, q):
        src, dst, to = (
            (p1.at[lax.rem(q, 2), 3], dr.at[q, 3], partner),
            (p0.at[q, 3, lo], ri.at[q, 0], right),
            (p0.at[q, 3, hi], ri.at[q, 1], left),
            (p0.at[q, 2, hi], fl.at[q, hi], right),
            (p0.at[q, 1, lo], fr.at[q, lo], left),
            (p0.at[q, 2, lo], fl.at[q, lo], right),
            (p0.at[q, 1, hi], fr.at[q, hi], left),
            (p1.at[lax.rem(q, 2), pl.ds(0, 3)], dr.at[q, pl.ds(0, 3)], partner),
        )[k]
        return pltpu.make_async_remote_copy(src_ref=src, dst_ref=dst, send_sem=rs_send.at[q, k], recv_sem=rs_recv.at[q, k],
                                            device_id={'ep': to}, device_id_type=pl.DeviceIdType.MESH)

    def ag_own(m):
        for k in range(4):
            ag(m, k).start()

    def ag_relay(m):
        ag(m, 0).wait_recv()
        ag(m, 5).start()
        ag(m, 2).wait_recv()
        ag(m, 6).start()

    def ag_share(m):
        ag(m, 1).wait_recv()
        ag(m, 7).start()
        ag(m, 3).wait_recv()
        ag(m, 8).start()

    def ag_share_far(m):
        ag(m, 5).wait_recv()
        ag(m, 9).start()
        ag(m, 6).wait_recv()
        ag(m, 10).start()

    lane = lax.broadcasted_iota(jnp.int32, (local_n, n_slot), 1)
    owner = lax.broadcasted_iota(jnp.int32, (local_n, n_slot), 0)
    spread = jnp.where((lane >= owner * cap) & (lane < (owner + 1) * cap), 1.0, 0.0).astype(F32)

    def member_gate(m, o, j):
        ids = lax.broadcasted_iota(jnp.int32, (local_n, tok_n), 0).astype(F32) + first
        member = jnp.zeros((local_n, tok_n), F32)
        gate = jnp.zeros((local_n, tok_n), F32)
        for t in range(top_k):
            hit = mbuf[o, j, 16 * m + t:16 * m + t + 1, :] == ids
            member = jnp.where(hit, 1.0, member)
            gate = jnp.where(hit, mbuf[o, j, 16 * m + 8 + t:16 * m + 9 + t, :], gate)
        return member, gate

    def locate(m, o):
        tri = jnp.where(lax.broadcasted_iota(jnp.int32, (tok_n, tok_n), 0) < lax.broadcasted_iota(jnp.int32, (tok_n, tok_n), 1),
                        1.0, 0.0).astype(BF16)
        for j in range(2):
            member, _ = member_gate(m, o, j)
            rank = jnp.dot(member.astype(BF16), tri, preferred_element_type=F32)
            slots[o, :, j * tok_n:(j + 1) * tok_n] = jnp.where(member > 0.5, rank + float(j * cap), -1.0)

    def take(o, e0, e1):
        index = lax.broadcasted_iota(jnp.int32, (cap2, 2 * tok_n), 0).astype(F32)
        sel = jnp.concatenate([jnp.where(index == slots[o, e:e + 1, :], 1.0, 0.0) for e in range(e0, e1)], axis=0).astype(BF16)
        wide = 2 * WIDE
        both = xbuf[o].reshape(2 * tok_n, dim)
        for k in range(0, dim, wide):
            n = min(wide, dim - k)
            got = jnp.dot(sel, both[:, k:k + n], preferred_element_type=F32).astype(BF16)
            for e in range(e1 - e0):
                rows[e, o * cap2:(o + 1) * cap2, k:k + n] = got[e * cap2:(e + 1) * cap2, :]

    def weigh(m, o):
        pos = lax.rem(lax.broadcasted_iota(jnp.int32, (tok_n, n_slot), 1), cap).astype(F32)

        def over(a):
            return lax.dot_general(a, spread, (((0,), (0,)), ((), ())), preferred_element_type=F32)

        for j in range(2):
            member, rest = member_gate(m, o, j)
            slot = slots[o, :, j * tok_n:(j + 1) * tok_n]
            here = over(jnp.where(member > 0.5, slot - float(j * cap), -1.0)) == pos
            for part in range(3):
                head = rest.astype(BF16).astype(F32)
                gts[o, j, part * tok_n:(part + 1) * tok_n, :] = jnp.where(here, over(head), 0.0).astype(BF16)
                rest = rest - head

    def gate_up(base, begin, end, kinds, events, both=False):
        def act(mine, at):
            gate = jnp.dot(mine, ring[lax.rem(at, RING)], preferred_element_type=F32)
            up = jnp.dot(mine, ring[lax.rem(at + 1, RING)], preferred_element_type=F32)
            return (jax.nn.silu(gate) * up).astype(BF16)

        def step(i, carry):
            at = base + 2 * i
            e, f = i // n_f, i % n_f
            tall_copy(wo_ref.at[:, pl.ds(0, WIDE)], at).wait()
            tall_copy(wo_ref.at[:, pl.ds(0, WIDE)], at + 1).wait()
            hidden[e, :, cols(f)] = act(rows[e], at)
            if both:
                k = e - (local_n - SHARED)
                later[k, :, cols(f)] = act(rows[k], at)
            fetch(at + RING, kinds)
            fetch(at + 1 + RING, kinds)
            events(i)
            return carry

        lax.fori_loop(begin, end, step, 0)

    def far_add(q):
        rs(0, q).wait_recv()
        p0[q, 3] = p0[q, 3] + dr[q, 3]

    def far_send(q):
        for k in (1, 2):
            rs(k, q).start()

    def stage1(q):
        rs(7, q).wait_recv()
        for o in (2, 1, 0):
            p0[q, o] = p0[q, o] + dr[q, o]
        for k in (3, 4):
            rs(k, q).start()

    def stage2(q):
        rs(1, q).wait_recv()
        rs(2, q).wait_recv()
        p0[q, 2, lo] = p0[q, 2, lo] + ri[q, 0]
        p0[q, 1, hi] = p0[q, 1, hi] + ri[q, 1]
        rs(5, q).start()
        rs(6, q).start()

    def combine(q, ready):
        for o in (3, 2, 1, 0):
            for j in (1, 0):
                parts = jnp.dot(gts[o, j], ys[o, j], preferred_element_type=F32)
                total = parts[:tok_n] + parts[tok_n:2 * tok_n] + parts[2 * tok_n:]
                if j == 1:
                    p1[lax.rem(q, 2), o] = total
                else:
                    p0[q, o] = total
            if o == 3:
                ready()
                rs(0, q).start()
        rs(7, q).start()

    def down(m, base, kinds):
        n_e = local_n // 2

        def step(i, carry):
            at = base + 2 * i
            q, e = i // n_e, i % n_e
            down_copy(0, 0, at).wait()
            down_copy(0, 0, at + 1).wait()
            y0 = jnp.dot(hidden[2 * e], ring[lax.rem(at, RING), pl.ds(0, ff)], preferred_element_type=F32)
            y1 = jnp.dot(hidden[2 * e + 1], ring[lax.rem(at + 1, RING), pl.ds(0, ff)], preferred_element_type=F32)
            for o in range(n_pair):
                for j in range(2):
                    here = slice(o * cap2 + j * cap, o * cap2 + (j + 1) * cap)
                    two = jnp.concatenate([y0[here], y1[here]], axis=0)
                    ys[o, j, pl.ds(pl.multiple_of(e * cap2, 16), cap2), :] = two.astype(BF16)
            far = (e == 0) & (q >= 1)

            @pl.when(far)
            def _():
                far_add(q - 1)

            fetch(at + RING, kinds)
            fetch(at + 1 + RING, kinds)

            @pl.when(far)
            def _():
                far_send(q - 1)

            if m == 1:
                @pl.when(e == 0)
                def _():
                    finish(0, q)
                    for peer in peers:
                        pl.semaphore_signal(rs_free.at[q], inc=1, device_id={'ep': peer}, device_id_type=pl.DeviceIdType.MESH)

            @pl.when((e == 1) & (q >= 1))
            def _():
                stage1(q - 1)

            @pl.when(e == n_e - 1)
            def _():
                @pl.when(q >= 2)
                def _():
                    rs(0, q - 2).wait_send()
                    rs(7, q - 2).wait_send()

                def ready():
                    if m == 1:
                        pl.semaphore_wait(rs_free.at[q], len(peers))

                combine(q, ready)
            return carry

        lax.fori_loop(0, n_d // 2, step, 0)

    def finish(m, q):
        for k in (3, 4, 5, 6):
            rs(k, q).wait_recv()
        total = p0[q, 0] + fl[q] + fr[q]
        tokens, out = (abuf, abuf) if m == 0 else (ubuf, bbuf)
        out[:, cols(q)] = (tokens[:, cols(q)].astype(F32) + total).astype(BF16)
        for k in (1, 2, 3, 4, 5, 6):
            rs(k, q).wait_send()

    def io(k):
        src, dst = (
            (x_ref, xbuf.at[0, 0]),
            (attn_ref, bbuf),
            (h_ref, hbuf),
            (x_ref, abuf),
            (abuf, outa_ref),
            (bbuf, outb_ref),
            (xbuf.at[0, 0], qkv_ref.at[:, pl.ds(0, dim)]),
            (xbuf.at[1, 0, :, pl.ds(0, qkv_n - dim)], qkv_ref.at[:, pl.ds(dim, qkv_n - dim)]),
        )[k]
        return pltpu.make_async_copy(src, dst, io_sem.at[k])

    for k in range(3):
        io(k).start()
    for idx in range(RING):
        fetch(idx, ('o', 'ga'))
    barrier = pltpu.get_barrier_semaphore()
    signal_peers(barrier)
    mbuf[0, 0] = jnp.zeros_like(mbuf[0, 0])
    for at, ref in ((0, ra_ref), (8, ga_ref), (16, rb_ref), (24, gb_ref)):
        mbuf[0, 0, at:at + top_k, :] = ref[...].astype(F32)
    io(0).wait()
    pl.semaphore_wait(barrier, len(peers))
    for k in (0, 1, 2):
        meta(k).start()
    ag_own(0)
    ag(0, 4).start()
    io(1).wait()
    io(2).wait()
    io(3).start()

    def project(i, carry):
        proj = jnp.dot(bbuf[...], tall(i), preferred_element_type=F32).astype(BF16)
        ubuf[:, cols(i)] = (hbuf[:, cols(i)].astype(F32) + proj.astype(F32)).astype(BF16)
        fetch(i + RING, ('ga',))
        return carry

    lax.fori_loop(0, n_o, project, 0)
    meta(0).wait_recv()
    meta(3).start()
    meta(4).start()
    meta(1).wait_recv()
    meta(5).start()
    meta(2).wait_recv()
    ag(0, 4).wait_recv()
    locate(0, 0)
    take(0, 0, local_n)
    ag_relay(0)
    ag_own(1)
    meta(3).wait_recv()
    meta(6).start()
    for k in (4, 5, 6):
        meta(k).wait_recv()
    for o in range(1, n_pair):
        locate(0, o)
    ag_share(0)
    ag(0, 7).wait_recv()
    take(1, 0, local_n)
    ag(0, 8).wait_recv()
    take(2, 0, local_n)
    ag_share_far(0)
    ag(0, 9).wait_recv()
    ag(0, 10).wait_recv()
    take(3, 0, local_n)
    for k in range(11):
        ag(0, k).wait_send()
    for k in range(7):
        meta(k).wait_send()
    signal_peers(x_free)
    xbuf[0, 0] = ubuf[...]

    def relay_b():
        pl.semaphore_wait(x_free, len(peers))
        ag(1, 4).start()
        ag_relay(1)

    def during_a(i):
        for when, event in ((6, relay_b), (11, lambda: ag_share(1)), (16, lambda: ag_share_far(1))):
            @pl.when(i == when)
            def _():
                event()

        @pl.when((i >= 7) & (i < 7 + n_pair))
        def _():
            weigh(0, i - 7)

    alone = (local_n - SHARED) * n_f
    gate_up(at_ga, 0, alone, ('ga', 'da'), during_a)
    for k in (4, 7, 8, 9, 10):
        ag(1, k).wait_recv()
    for o in range(n_pair):
        if o in (1, 2):
            xbuf[o, 0] = near[o - 1]
        locate(1, o)
        take(o, local_n - SHARED, local_n)
    gate_up(at_ga, alone, n_ga, ('ga', 'da'), lambda i: None, both=True)
    down(0, at_da, ('da', 'gb'))
    for o in range(n_pair):
        take(o, 0, local_n - SHARED)
        if o == 0:
            far_add(n_q - 1)
        if o == 1:
            far_send(n_q - 1)
            stage1(n_q - 1)
    for k in range(SHARED):
        hidden[local_n - SHARED + k] = later[k]
    for q in (n_q - 2, n_q - 1):
        rs(0, q).wait_send()
        rs(7, q).wait_send()

    def during_b(i):
        @pl.when((i % 3 == 2) & (i < 3 * n_q))
        def _():
            stage2(i // 3)

        @pl.when((i >= 12) & (i < 12 + n_pair))
        def _():
            weigh(1, i - 12)

    io(3).wait()
    gate_up(at_gb, 0, n_gb, ('gb', 'db'), during_b)
    down(1, at_db, ('db', 'w'))
    io(4).start()

    def qkv(i, carry):
        xbuf[i // n_o, 0, :, cols(i % n_o)] = jnp.dot(hbuf[...], tall(at_w + i), preferred_element_type=F32).astype(BF16)

        @pl.when(i == 0)
        def _():
            far_add(n_q - 1)

        @pl.when(i == 1)
        def _():
            far_send(n_q - 1)
            stage1(n_q - 1)

        @pl.when((i >= 2) & (i - 2 < n_q - 1))
        def _():
            stage2(i - 2)
        return carry

    lax.fori_loop(0, n_w, qkv, 0)
    io(6).start()
    io(7).start()
    stage2(n_q - 1)

    def last(q, carry):
        finish(1, q)
        return carry

    lax.fori_loop(0, n_q, last, 0)
    io(5).start()
    for q in (n_q - 2, n_q - 1):
        rs(0, q).wait_send()
        rs(7, q).wait_send()
    for k in range(11):
        ag(1, k).wait_send()
    for k in (4, 5, 6, 7):
        io(k).wait()


def write_kernel(a_ref, b_ref, c_ref, oa_ref, ob_ref, oc_ref, va, vb, vc, sem_in, sem_out):
    moves = ((a_ref, va, oa_ref), (b_ref, vb, ob_ref), (c_ref, vc, oc_ref))
    for k, (src, buf, _) in enumerate(moves):
        pltpu.make_async_copy(src, buf, sem_in.at[k]).start()
    for k, (src, buf, dst) in enumerate(moves):
        pltpu.make_async_copy(src, buf, sem_in.at[k]).wait()
        pltpu.make_async_copy(buf, dst, sem_out.at[k]).start()
    for k, (_, buf, dst) in enumerate(moves):
        pltpu.make_async_copy(buf, dst, sem_out.at[k]).wait()


def write_out(arrays):
    hbm = pl.BlockSpec(memory_space=pl.ANY)
    return pl.pallas_call(
        write_kernel,
        out_shape=tuple(jax.ShapeDtypeStruct(a.shape, a.dtype) for a in arrays),
        in_specs=[hbm] * 3,
        out_specs=(hbm,) * 3,
        scratch_shapes=[pltpu.VMEM(a.shape, a.dtype) for a in arrays] + [pltpu.SemaphoreType.DMA((3,)), pltpu.SemaphoreType.DMA((3,))],
    )(*arrays)


def solution(mesh):
    n_devs = mesh.shape['ep']

    def local_step(x_a, route_a, gate_a, h_b, attn_b, route_b, gate_b, w_qkv, w_o, w_gate, w_up, w_down):
        tok_n, dim = x_a.shape
        top_k = route_a.shape[1]
        local_n, _, ff = w_gate.shape
        qkv_n = w_qkv.shape[1]
        n_experts = local_n * n_devs
        cap = min(tok_n, 2 * ((tok_n * top_k + n_experts - 1) // n_experts))
        n_pair = n_devs // 2
        n_q = dim // WIDE
        cap2 = 2 * cap
        m = n_pair * cap2
        half = tok_n // 2

        vmem = pl.BlockSpec(memory_space=pltpu.VMEM)
        hbm = pl.BlockSpec(memory_space=pl.ANY)
        flops = 2 * 2 * 3 * local_n * m * dim * ff
        weight_bytes = 2 * 6 * local_n * dim * ff
        results = pl.pallas_call(
            functools.partial(moe_kernel, n_devs, top_k, cap),
            out_shape=(
                jax.ShapeDtypeStruct((tok_n, dim), BF16),
                jax.ShapeDtypeStruct((tok_n, dim), BF16),
                jax.ShapeDtypeStruct((tok_n, qkv_n), BF16),
            ),
            in_specs=[vmem] * 4 + [hbm] * 8,
            out_specs=(hbm, hbm, hbm),
            scratch_shapes=[
                pltpu.VMEM((RING, dim, WIDE), BF16),
                pltpu.VMEM((n_pair, 2, tok_n, dim), BF16),
                pltpu.VMEM((2, tok_n, dim), BF16),
                pltpu.VMEM((n_pair, 2, 32, tok_n), F32),
                pltpu.VMEM((tok_n, dim), BF16),
                pltpu.VMEM((tok_n, dim), BF16),
                pltpu.VMEM((tok_n, dim), BF16),
                pltpu.VMEM((tok_n, dim), BF16),
                pltpu.VMEM((local_n, m, dim), BF16),
                pltpu.VMEM((local_n, m, ff), BF16),
                pltpu.VMEM((SHARED, m, ff), BF16),
                pltpu.VMEM((n_pair, local_n, 2 * tok_n), F32),
                pltpu.VMEM((n_pair, 2, 3 * tok_n, local_n * cap), BF16),
                pltpu.VMEM((n_pair, 2, local_n * cap, WIDE), BF16),
                pltpu.VMEM((n_q, n_pair, tok_n, WIDE), F32),
                pltpu.VMEM((2, n_pair, tok_n, WIDE), F32),
                pltpu.VMEM((n_q, n_pair, tok_n, WIDE), F32),
                pltpu.VMEM((n_q, 2, half, WIDE), F32),
                pltpu.VMEM((n_q, tok_n, WIDE), F32),
                pltpu.VMEM((n_q, tok_n, WIDE), F32),
                pltpu.SemaphoreType.DMA((RING,)),
                pltpu.SemaphoreType.DMA((8,)),
                pltpu.SemaphoreType.DMA((2, 11)),
                pltpu.SemaphoreType.DMA((2, 11)),
                pltpu.SemaphoreType.DMA((7,)),
                pltpu.SemaphoreType.DMA((7,)),
                pltpu.SemaphoreType.DMA((n_q, 8)),
                pltpu.SemaphoreType.DMA((n_q, 8)),
                pltpu.SemaphoreType.REGULAR,
                pltpu.SemaphoreType.REGULAR((n_q,)),
            ],
            compiler_params=pltpu.CompilerParams(collective_id=0, has_side_effects=True, vmem_limit_bytes=67043328),
            cost_estimate=pl.CostEstimate(flops=flops, bytes_accessed=weight_bytes, transcendentals=0),
        )(route_a.T, gate_a.T, route_b.T, gate_b.T, x_a, h_b, attn_b, w_qkv, w_o, w_gate, w_up, w_down)
        return write_out(results)

    row_spec = P(('dp', 'ep'), None)
    full_spec = P(None, None)
    expert_spec = P('ep', None, None)
    return jax.shard_map(
        local_step,
        mesh=mesh,
        in_specs=(row_spec, row_spec, row_spec, row_spec, row_spec, row_spec, row_spec, full_spec, full_spec, expert_spec, expert_spec, expert_spec),
        out_specs=(row_spec, row_spec, row_spec),
        check_vma=False,
    )
```

```python
import functools

import jax
import jax.numpy as jnp
from jax import lax
from jax.experimental import pallas as pl
from jax.experimental.pallas import tpu as pltpu
from jax.sharding import PartitionSpec as P

F32 = jnp.float32
BF16 = jnp.bfloat16
RING = 8
WIDE = 512
SHARED = 2


def moe_kernel(n_devs, top_k, cap, ra_ref, ga_ref, rb_ref, gb_ref, x_ref, h_ref, attn_ref,
               wqkv_ref, wo_ref, wg_ref, wu_ref, wd_ref,
               outa_ref, outb_ref, qkv_ref,
               ring, xbuf, near, mbuf, ubuf, abuf, bbuf, hbuf, rows, hidden, later, slots, gts, ys, p0, p1, dr, ri, fl, fr,
               ring_sem, io_sem, ag_send, ag_recv, me_send, me_recv, rs_send, rs_recv, x_free, rs_free):
    tok_n, dim = x_ref.shape
    half = tok_n // 2
    local_n, _, ff = wg_ref.shape
    qkv_n = wqkv_ref.shape[1]
    cap2 = 2 * cap
    n_pair = n_devs // 2
    n_slot = local_n * cap
    me = lax.axis_index('ep')
    core = lax.rem(me, 2)
    partner = me + 1 - 2 * core
    right = lax.rem(me + 2, n_devs)
    left = lax.rem(me + n_devs - 2, n_devs)
    first = (me * local_n).astype(F32)
    peers = (partner, left, right)

    def signal_peers(sem):
        for peer in peers:
            pl.semaphore_signal(sem, inc=1, device_id={'ep': peer}, device_id_type=pl.DeviceIdType.MESH)

    n_o, n_f, n_q, n_w = dim // WIDE, ff // WIDE, dim // WIDE, qkv_n // WIDE
    n_ga, n_gb, n_d = local_n * n_f, (local_n - SHARED) * n_f, local_n * n_q
    at_ga = n_o
    at_da = at_ga + 2 * n_ga
    at_gb = at_da + n_d
    at_db = at_gb + 2 * n_gb
    at_w = at_db + n_d
    at_end = at_w + n_w

    def cols(k):
        return pl.ds(pl.multiple_of(k * WIDE, WIDE), WIDE)

    def tall_copy(src, idx):
        slot = lax.rem(idx, RING)
        return pltpu.make_async_copy(src, ring.at[slot], ring_sem.at[slot])

    def down_copy(e, k, idx):
        slot = lax.rem(idx, RING)
        return pltpu.make_async_copy(wd_ref.at[e, :, cols(k)], ring.at[slot, pl.ds(0, ff)], ring_sem.at[slot])

    def start_gu(t, idx):
        step = t // 2
        e, f = step // n_f, step % n_f

        @pl.when(t % 2 == 0)
        def _():
            tall_copy(wg_ref.at[e, :, cols(f)], idx).start()

        @pl.when(t % 2 == 1)
        def _():
            tall_copy(wu_ref.at[e, :, cols(f)], idx).start()

    def fetch(idx, kinds):
        if 'o' in kinds:
            @pl.when(idx < at_ga)
            def _():
                tall_copy(wo_ref.at[:, cols(idx)], idx).start()
        for name, base, steps in (('ga', at_ga, n_ga), ('gb', at_gb, n_gb)):
            if name in kinds:
                @pl.when((idx >= base) & (idx < base + 2 * steps))
                def _():
                    start_gu(idx - base, idx)
        for name, base in (('da', at_da), ('db', at_db)):
            if name in kinds:
                @pl.when((idx >= base) & (idx < base + n_d))
                def _():
                    t = idx - base
                    down_copy(t % local_n, t // local_n, idx).start()
        if 'w' in kinds:
            @pl.when((idx >= at_w) & (idx < at_end))
            def _():
                tall_copy(wqkv_ref.at[:, cols(idx - at_w)], idx).start()

    def tall(idx):
        tall_copy(wo_ref.at[:, pl.ds(0, WIDE)], idx).wait()
        return ring[lax.rem(idx, RING)]

    lo, hi = pl.ds(0, half), pl.ds(half, half)

    def ag(m, k):
        own, from_left, from_right = (xbuf.at[0, 0], xbuf.at[1, 0], xbuf.at[2, 0]) if m == 0 else (ubuf, near.at[0], near.at[1])
        src, dst, to = (
            (own.at[lo], from_left.at[lo], right),
            (own.at[hi], from_left.at[hi], right),
            (own.at[hi], from_right.at[hi], left),
            (own.at[lo], from_right.at[lo], left),
            (own, xbuf.at[0, 1], partner),
            (from_left.at[lo], xbuf.at[3, 0, lo], right),
            (from_right.at[hi], xbuf.at[3, 0, hi], left),
            (from_left, xbuf.at[1, 1], partner),
            (from_right, xbuf.at[2, 1], partner),
            (xbuf.at[3, 0, lo], xbuf.at[3, 1, lo], partner),
            (xbuf.at[3, 0, hi], xbuf.at[3, 1, hi], partner),
        )[k]
        return pltpu.make_async_remote_copy(src_ref=src, dst_ref=dst, send_sem=ag_send.at[m, k], recv_sem=ag_recv.at[m, k],
                                            device_id={'ep': to}, device_id_type=pl.DeviceIdType.MESH)

    def meta(k):
        src, dst, to = (
            (mbuf.at[0, 0], mbuf.at[1, 0], right),
            (mbuf.at[0, 0], mbuf.at[2, 0], left),
            (mbuf.at[0, 0], mbuf.at[0, 1], partner),
            (mbuf.at[1, 0], mbuf.at[3, 0], right),
            (mbuf.at[1, 0], mbuf.at[1, 1], partner),
            (mbuf.at[2, 0], mbuf.at[2, 1], partner),
            (mbuf.at[3, 0], mbuf.at[3, 1], partner),
        )[k]
        return pltpu.make_async_remote_copy(src_ref=src, dst_ref=dst, send_sem=me_send.at[k], recv_sem=me_recv.at[k],
                                            device_id={'ep': to}, device_id_type=pl.DeviceIdType.MESH)

    def rs(k, q):
        src, dst, to = (
            (p1.at[lax.rem(q, 2), 3], dr.at[q, 3], partner),
            (p0.at[q, 3, lo], ri.at[q, 0], right),
            (p0.at[q, 3, hi], ri.at[q, 1], left),
            (p0.at[q, 2, hi], fl.at[q, hi], right),
            (p0.at[q, 1, lo], fr.at[q, lo], left),
            (p0.at[q, 2, lo], fl.at[q, lo], right),
            (p0.at[q, 1, hi], fr.at[q, hi], left),
            (p1.at[lax.rem(q, 2), pl.ds(0, 3)], dr.at[q, pl.ds(0, 3)], partner),
        )[k]
        return pltpu.make_async_remote_copy(src_ref=src, dst_ref=dst, send_sem=rs_send.at[q, k], recv_sem=rs_recv.at[q, k],
                                            device_id={'ep': to}, device_id_type=pl.DeviceIdType.MESH)

    def ag_own(m):
        for k in range(4):
            ag(m, k).start()

    def ag_relay(m):
        ag(m, 0).wait_recv()
        ag(m, 5).start()
        ag(m, 2).wait_recv()
        ag(m, 6).start()

    def ag_share(m):
        ag(m, 1).wait_recv()
        ag(m, 7).start()
        ag(m, 3).wait_recv()
        ag(m, 8).start()

    def ag_share_far(m):
        ag(m, 5).wait_recv()
        ag(m, 9).start()
        ag(m, 6).wait_recv()
        ag(m, 10).start()

    lane = lax.broadcasted_iota(jnp.int32, (local_n, n_slot), 1)
    owner = lax.broadcasted_iota(jnp.int32, (local_n, n_slot), 0)
    spread = jnp.where((lane >= owner * cap) & (lane < (owner + 1) * cap), 1.0, 0.0).astype(F32)

    def member_gate(m, o, j):
        ids = lax.broadcasted_iota(jnp.int32, (local_n, tok_n), 0).astype(F32) + first
        member = jnp.zeros((local_n, tok_n), F32)
        gate = jnp.zeros((local_n, tok_n), F32)
        for t in range(top_k):
            hit = mbuf[o, j, 16 * m + t:16 * m + t + 1, :] == ids
            member = jnp.where(hit, 1.0, member)
            gate = jnp.where(hit, mbuf[o, j, 16 * m + 8 + t:16 * m + 9 + t, :], gate)
        return member, gate

    def locate(m, o):
        tri = jnp.where(lax.broadcasted_iota(jnp.int32, (tok_n, tok_n), 0) < lax.broadcasted_iota(jnp.int32, (tok_n, tok_n), 1),
                        1.0, 0.0).astype(BF16)
        for j in range(2):
            member, _ = member_gate(m, o, j)
            rank = jnp.dot(member.astype(BF16), tri, preferred_element_type=F32)
            slots[o, :, j * tok_n:(j + 1) * tok_n] = jnp.where(member > 0.5, rank + float(j * cap), -1.0)

    def take(o, e0, e1):
        index = lax.broadcasted_iota(jnp.int32, (cap2, 2 * tok_n), 0).astype(F32)
        sel = jnp.concatenate([jnp.where(index == slots[o, e:e + 1, :], 1.0, 0.0) for e in range(e0, e1)], axis=0).astype(BF16)
        wide = 2 * WIDE
        both = xbuf[o].reshape(2 * tok_n, dim)
        for k in range(0, dim, wide):
            n = min(wide, dim - k)
            got = jnp.dot(sel, both[:, k:k + n], preferred_element_type=F32).astype(BF16)
            for e in range(e1 - e0):
                rows[e, o * cap2:(o + 1) * cap2, k:k + n] = got[e * cap2:(e + 1) * cap2, :]

    def weigh(m, o):
        pos = lax.rem(lax.broadcasted_iota(jnp.int32, (tok_n, n_slot), 1), cap).astype(F32)

        def over(a):
            return lax.dot_general(a, spread, (((0,), (0,)), ((), ())), preferred_element_type=F32)

        for j in range(2):
            member, rest = member_gate(m, o, j)
            slot = slots[o, :, j * tok_n:(j + 1) * tok_n]
            here = over(jnp.where(member > 0.5, slot - float(j * cap), -1.0)) == pos
            for part in range(3):
                head = rest.astype(BF16).astype(F32)
                gts[o, j, part * tok_n:(part + 1) * tok_n, :] = jnp.where(here, over(head), 0.0).astype(BF16)
                rest = rest - head

    def gate_up(base, begin, end, kinds, events, both=False):
        def act(mine, at):
            gate = jnp.dot(mine, ring[lax.rem(at, RING)], preferred_element_type=F32)
            up = jnp.dot(mine, ring[lax.rem(at + 1, RING)], preferred_element_type=F32)
            return (jax.nn.silu(gate) * up).astype(BF16)

        def step(i, carry):
            at = base + 2 * i
            e, f = i // n_f, i % n_f
            tall_copy(wo_ref.at[:, pl.ds(0, WIDE)], at).wait()
            tall_copy(wo_ref.at[:, pl.ds(0, WIDE)], at + 1).wait()
            hidden[e, :, cols(f)] = act(rows[e], at)
            if both:
                k = e - (local_n - SHARED)
                later[k, :, cols(f)] = act(rows[k], at)
            fetch(at + RING, kinds)
            fetch(at + 1 + RING, kinds)
            events(i)
            return carry

        lax.fori_loop(begin, end, step, 0)

    def far_add(q):
        rs(0, q).wait_recv()
        p0[q, 3] = p0[q, 3] + dr[q, 3]

    def far_send(q):
        for k in (1, 2):
            rs(k, q).start()

    def stage1(q):
        rs(7, q).wait_recv()
        for o in (2, 1, 0):
            p0[q, o] = p0[q, o] + dr[q, o]
        for k in (3, 4):
            rs(k, q).start()

    def stage2(q):
        rs(1, q).wait_recv()
        rs(2, q).wait_recv()
        p0[q, 2, lo] = p0[q, 2, lo] + ri[q, 0]
        p0[q, 1, hi] = p0[q, 1, hi] + ri[q, 1]
        rs(5, q).start()
        rs(6, q).start()

    def combine(q, ready):
        for o in (3, 2, 1, 0):
            for j in (1, 0):
                parts = jnp.dot(gts[o, j], ys[o, j], preferred_element_type=F32)
                total = parts[:tok_n] + parts[tok_n:2 * tok_n] + parts[2 * tok_n:]
                if j == 1:
                    p1[lax.rem(q, 2), o] = total
                else:
                    p0[q, o] = total
            if o == 3:
                ready()
                rs(0, q).start()
        rs(7, q).start()

    def down(m, base, kinds):
        n_e = local_n // 2

        def step(i, carry):
            at = base + 2 * i
            q, e = i // n_e, i % n_e
            down_copy(0, 0, at).wait()
            down_copy(0, 0, at + 1).wait()
            y0 = jnp.dot(hidden[2 * e], ring[lax.rem(at, RING), pl.ds(0, ff)], preferred_element_type=F32)
            y1 = jnp.dot(hidden[2 * e + 1], ring[lax.rem(at + 1, RING), pl.ds(0, ff)], preferred_element_type=F32)
            for o in range(n_pair):
                for j in range(2):
                    here = slice(o * cap2 + j * cap, o * cap2 + (j + 1) * cap)
                    two = jnp.concatenate([y0[here], y1[here]], axis=0)
                    ys[o, j, pl.ds(pl.multiple_of(e * cap2, 16), cap2), :] = two.astype(BF16)
            far = (e == 0) & (q >= 1)

            @pl.when(far)
            def _():
                far_add(q - 1)

            fetch(at + RING, kinds)
            fetch(at + 1 + RING, kinds)

            @pl.when(far)
            def _():
                far_send(q - 1)

            if m == 1:
                @pl.when(e == 0)
                def _():
                    finish(0, q)
                    for peer in peers:
                        pl.semaphore_signal(rs_free.at[q], inc=1, device_id={'ep': peer}, device_id_type=pl.DeviceIdType.MESH)

            @pl.when((e == 1) & (q >= 1))
            def _():
                stage1(q - 1)

            @pl.when(e == n_e - 1)
            def _():
                @pl.when(q >= 2)
                def _():
                    rs(0, q - 2).wait_send()
                    rs(7, q - 2).wait_send()

                def ready():
                    if m == 1:
                        pl.semaphore_wait(rs_free.at[q], len(peers))

                combine(q, ready)
            return carry

        lax.fori_loop(0, n_d // 2, step, 0)

    def finish(m, q):
        for k in (3, 4, 5, 6):
            rs(k, q).wait_recv()
        total = p0[q, 0] + fl[q] + fr[q]
        tokens, out = (abuf, abuf) if m == 0 else (ubuf, bbuf)
        out[:, cols(q)] = (tokens[:, cols(q)].astype(F32) + total).astype(BF16)
        for k in (1, 2, 3, 4, 5, 6):
            rs(k, q).wait_send()

    def io(k):
        src, dst = (
            (x_ref, xbuf.at[0, 0]),
            (attn_ref, bbuf),
            (h_ref, hbuf),
            (x_ref, abuf),
            (abuf, outa_ref),
            (bbuf, outb_ref),
            (xbuf.at[0, 0], qkv_ref.at[:, pl.ds(0, dim)]),
            (xbuf.at[1, 0, :, pl.ds(0, qkv_n - dim)], qkv_ref.at[:, pl.ds(dim, qkv_n - dim)]),
        )[k]
        return pltpu.make_async_copy(src, dst, io_sem.at[k])

    for k in range(3):
        io(k).start()
    for idx in range(RING):
        fetch(idx, ('o', 'ga'))
    barrier = pltpu.get_barrier_semaphore()
    signal_peers(barrier)
    mbuf[0, 0] = jnp.zeros_like(mbuf[0, 0])
    for at, ref in ((0, ra_ref), (8, ga_ref), (16, rb_ref), (24, gb_ref)):
        mbuf[0, 0, at:at + top_k, :] = ref[...].astype(F32)
    io(0).wait()
    pl.semaphore_wait(barrier, len(peers))
    for k in (0, 1, 2):
        meta(k).start()
    ag_own(0)
    ag(0, 4).start()
    io(1).wait()
    io(2).wait()
    io(3).start()

    def project(i, carry):
        proj = jnp.dot(bbuf[...], tall(i), preferred_element_type=F32).astype(BF16)
        ubuf[:, cols(i)] = (hbuf[:, cols(i)].astype(F32) + proj.astype(F32)).astype(BF16)
        fetch(i + RING, ('ga',))
        return carry

    lax.fori_loop(0, n_o, project, 0)
    meta(0).wait_recv()
    meta(3).start()
    meta(4).start()
    meta(1).wait_recv()
    meta(5).start()
    meta(2).wait_recv()
    ag(0, 4).wait_recv()
    locate(0, 0)
    take(0, 0, local_n)
    ag_relay(0)
    ag_own(1)
    meta(3).wait_recv()
    meta(6).start()
    for k in (4, 5, 6):
        meta(k).wait_recv()
    for o in range(1, n_pair):
        locate(0, o)
    ag_share(0)
    ag(0, 7).wait_recv()
    take(1, 0, local_n)
    ag(0, 8).wait_recv()
    take(2, 0, local_n)
    ag_share_far(0)
    ag(0, 9).wait_recv()
    ag(0, 10).wait_recv()
    take(3, 0, local_n)
    for k in range(11):
        ag(0, k).wait_send()
    for k in range(7):
        meta(k).wait_send()
    signal_peers(x_free)
    xbuf[0, 0] = ubuf[...]

    def relay_b():
        pl.semaphore_wait(x_free, len(peers))
        ag(1, 4).start()
        ag_relay(1)

    def during_a(i):
        for when, event in ((6, relay_b), (11, lambda: ag_share(1)), (16, lambda: ag_share_far(1))):
            @pl.when(i == when)
            def _():
                event()

        @pl.when((i >= 7) & (i < 7 + n_pair))
        def _():
            weigh(0, i - 7)

    alone = (local_n - SHARED) * n_f
    gate_up(at_ga, 0, alone, ('ga', 'da'), during_a)
    for k in (4, 7, 8, 9, 10):
        ag(1, k).wait_recv()
    for o in range(n_pair):
        if o in (1, 2):
            xbuf[o, 0] = near[o - 1]
        locate(1, o)
        take(o, local_n - SHARED, local_n)
    gate_up(at_ga, alone, n_ga, ('ga', 'da'), lambda i: None, both=True)
    down(0, at_da, ('da', 'gb'))
    for o in range(n_pair):
        take(o, 0, local_n - SHARED)
        if o == 0:
            far_add(n_q - 1)
        if o == 1:
            far_send(n_q - 1)
            stage1(n_q - 1)
    for k in range(SHARED):
        hidden[local_n - SHARED + k] = later[k]
    for q in (n_q - 2, n_q - 1):
        rs(0, q).wait_send()
        rs(7, q).wait_send()

    def during_b(i):
        @pl.when((i % 2 == 1) & (i < 2 * n_q))
        def _():
            stage2(i // 2)

        @pl.when((i >= 12) & (i < 12 + n_pair))
        def _():
            weigh(1, i - 12)

    io(3).wait()
    gate_up(at_gb, 0, n_gb, ('gb', 'db'), during_b)
    down(1, at_db, ('db', 'w'))
    io(4).start()

    def qkv(i, carry):
        xbuf[i // n_o, 0, :, cols(i % n_o)] = jnp.dot(hbuf[...], tall(at_w + i), preferred_element_type=F32).astype(BF16)

        @pl.when(i == 0)
        def _():
            far_add(n_q - 1)

        @pl.when(i == 1)
        def _():
            far_send(n_q - 1)
            stage1(n_q - 1)

        @pl.when((i >= 2) & (i - 2 < n_q - 1))
        def _():
            stage2(i - 2)
        return carry

    lax.fori_loop(0, n_w, qkv, 0)
    io(6).start()
    io(7).start()
    stage2(n_q - 1)

    def last(q, carry):
        finish(1, q)
        return carry

    lax.fori_loop(0, n_q, last, 0)
    io(5).start()
    for q in (n_q - 2, n_q - 1):
        rs(0, q).wait_send()
        rs(7, q).wait_send()
    for k in range(11):
        ag(1, k).wait_send()
    for k in (4, 5, 6, 7):
        io(k).wait()


def write_kernel(a_ref, b_ref, c_ref, oa_ref, ob_ref, oc_ref, va, vb, vc, sem_in, sem_out):
    moves = ((a_ref, va, oa_ref), (b_ref, vb, ob_ref), (c_ref, vc, oc_ref))
    for k, (src, buf, _) in enumerate(moves):
        pltpu.make_async_copy(src, buf, sem_in.at[k]).start()
    for k, (src, buf, dst) in enumerate(moves):
        pltpu.make_async_copy(src, buf, sem_in.at[k]).wait()
        pltpu.make_async_copy(buf, dst, sem_out.at[k]).start()
    for k, (_, buf, dst) in enumerate(moves):
        pltpu.make_async_copy(buf, dst, sem_out.at[k]).wait()


def write_out(arrays):
    hbm = pl.BlockSpec(memory_space=pl.ANY)
    return pl.pallas_call(
        write_kernel,
        out_shape=tuple(jax.ShapeDtypeStruct(a.shape, a.dtype) for a in arrays),
        in_specs=[hbm] * 3,
        out_specs=(hbm,) * 3,
        scratch_shapes=[pltpu.VMEM(a.shape, a.dtype) for a in arrays] + [pltpu.SemaphoreType.DMA((3,)), pltpu.SemaphoreType.DMA((3,))],
    )(*arrays)


def solution(mesh):
    n_devs = mesh.shape['ep']

    def local_step(x_a, route_a, gate_a, h_b, attn_b, route_b, gate_b, w_qkv, w_o, w_gate, w_up, w_down):
        tok_n, dim = x_a.shape
        top_k = route_a.shape[1]
        local_n, _, ff = w_gate.shape
        qkv_n = w_qkv.shape[1]
        n_experts = local_n * n_devs
        cap = min(tok_n, 2 * ((tok_n * top_k + n_experts - 1) // n_experts))
        n_pair = n_devs // 2
        n_q = dim // WIDE
        cap2 = 2 * cap
        m = n_pair * cap2
        half = tok_n // 2

        vmem = pl.BlockSpec(memory_space=pltpu.VMEM)
        hbm = pl.BlockSpec(memory_space=pl.ANY)
        flops = 2 * 2 * 3 * local_n * m * dim * ff
        weight_bytes = 2 * 6 * local_n * dim * ff
        results = pl.pallas_call(
            functools.partial(moe_kernel, n_devs, top_k, cap),
            out_shape=(
                jax.ShapeDtypeStruct((tok_n, dim), BF16),
                jax.ShapeDtypeStruct((tok_n, dim), BF16),
                jax.ShapeDtypeStruct((tok_n, qkv_n), BF16),
            ),
            in_specs=[vmem] * 4 + [hbm] * 8,
            out_specs=(hbm, hbm, hbm),
            scratch_shapes=[
                pltpu.VMEM((RING, dim, WIDE), BF16),
                pltpu.VMEM((n_pair, 2, tok_n, dim), BF16),
                pltpu.VMEM((2, tok_n, dim), BF16),
                pltpu.VMEM((n_pair, 2, 32, tok_n), F32),
                pltpu.VMEM((tok_n, dim), BF16),
                pltpu.VMEM((tok_n, dim), BF16),
                pltpu.VMEM((tok_n, dim), BF16),
                pltpu.VMEM((tok_n, dim), BF16),
                pltpu.VMEM((local_n, m, dim), BF16),
                pltpu.VMEM((local_n, m, ff), BF16),
                pltpu.VMEM((SHARED, m, ff), BF16),
                pltpu.VMEM((n_pair, local_n, 2 * tok_n), F32),
                pltpu.VMEM((n_pair, 2, 3 * tok_n, local_n * cap), BF16),
                pltpu.VMEM((n_pair, 2, local_n * cap, WIDE), BF16),
                pltpu.VMEM((n_q, n_pair, tok_n, WIDE), F32),
                pltpu.VMEM((2, n_pair, tok_n, WIDE), F32),
                pltpu.VMEM((n_q, n_pair, tok_n, WIDE), F32),
                pltpu.VMEM((n_q, 2, half, WIDE), F32),
                pltpu.VMEM((n_q, tok_n, WIDE), F32),
                pltpu.VMEM((n_q, tok_n, WIDE), F32),
                pltpu.SemaphoreType.DMA((RING,)),
                pltpu.SemaphoreType.DMA((8,)),
                pltpu.SemaphoreType.DMA((2, 11)),
                pltpu.SemaphoreType.DMA((2, 11)),
                pltpu.SemaphoreType.DMA((7,)),
                pltpu.SemaphoreType.DMA((7,)),
                pltpu.SemaphoreType.DMA((n_q, 8)),
                pltpu.SemaphoreType.DMA((n_q, 8)),
                pltpu.SemaphoreType.REGULAR,
                pltpu.SemaphoreType.REGULAR((n_q,)),
            ],
            compiler_params=pltpu.CompilerParams(collective_id=0, has_side_effects=True, vmem_limit_bytes=67043328),
            cost_estimate=pl.CostEstimate(flops=flops, bytes_accessed=weight_bytes, transcendentals=0),
        )(route_a.T, gate_a.T, route_b.T, gate_b.T, x_a, h_b, attn_b, w_qkv, w_o, w_gate, w_up, w_down)
        return write_out(results)

    row_spec = P(('dp', 'ep'), None)
    full_spec = P(None, None)
    expert_spec = P('ep', None, None)
    return jax.shard_map(
        local_step,
        mesh=mesh,
        in_specs=(row_spec, row_spec, row_spec, row_spec, row_spec, row_spec, row_spec, full_spec, full_spec, expert_spec, expert_spec, expert_spec),
        out_specs=(row_spec, row_spec, row_spec),
        check_vma=False,
    )
```
